32 devices in a mesh: tm: 8 (over y, x, core), strip: 4 (over z).
Axes of the slice: x: 2, y: 2, z: 4, core: 2. Of those that a mesh axis runs over, the one named last changes fastest.
Arguments:
- signal: bfloat16 [2, 16, 16384], P(None, 'strip', 'tm'), may hold values from -5 to 5
Outputs:
- spectrum: bfloat16 [2, 256, 16, 8, 2048], P(None, 'strip', None, 'tm')
The draws below stay inside these ranges and needn't reach their ends.
All inputs are finite; a program needn't handle non-finite values.
Results may differ from the reference program's by a relative error of at most 0.0069.
Values may be sent and summed in bfloat16 or wider, within the bound.
A program may use at most 128 MiB of HBM per device.

```python
import math
import jax
import jax.numpy as jnp
from jax import lax

K = 256
L = 16384
W = 16
NRES = 8
LB = 2048


def shard_levels(rng, shape, pieces, least, high):
    level = 1.0
    for axis_at, parts in pieces:
        draws = jax.random.uniform(jax.random.fold_in(jax.random.fold_in(rng, 6), axis_at), (parts,), jnp.float32, least / len(pieces), high / len(pieces))
        level = level * jnp.repeat(jnp.exp(draws), shape[axis_at] // parts).reshape((-1,) + (1,) * (len(shape) - 1 - axis_at))
    return level


def bell_draw(key, dims, deviation, bound, cuts=(), kind=jnp.bfloat16):
    result = deviation * jax.random.normal(key, dims, jnp.float32)
    if cuts:
        result = result * shard_levels(key, dims, cuts, -0.22, 0.18)
    return jnp.clip(result, -bound, bound).astype(kind)


def setup_inputs(seed: int = 0) -> dict:
    splits = jax.random.split(jax.random.key(seed), 2)
    return {
        "signal": bell_draw(splits[0], (2, W, L), 0.7, 5.0, ((1, 4), (2, 8))),
    }


TWO_PI = 2.0 * math.pi

def channel_filters(channel_ids, length):
    offsets = jnp.arange(length, dtype=jnp.int32)
    phases = channel_ids[:, None] * offsets[None, :] % length
    angles = jnp.float32(TWO_PI) * phases.astype(jnp.float32) / length
    hamming = 0.54 - 0.46 * jnp.cos(jnp.float32(TWO_PI) * offsets.astype(jnp.float32) / length)
    scaled = hamming[None, :] / math.sqrt(length)
    cosine = scaled * jnp.cos(angles)
    sine = scaled * jnp.sin(angles)
    real_rows = jnp.stack([cosine, sine], axis=1)
    imag_rows = jnp.stack([-sine, cosine], axis=1)
    return jnp.concatenate([real_rows, imag_rows], axis=0).astype(jnp.bfloat16)

def dft_pair(first, second, modulus, norm):
    phases = first[:, None] * second[None, :] % modulus
    angles = jnp.float32(TWO_PI) * phases.astype(jnp.float32) / modulus
    return (jnp.cos(angles) * norm, jnp.sin(angles) * norm)

def reference(signal):
    filters = channel_filters(jnp.arange(K, dtype=jnp.int32), K).astype(jnp.float32)
    res_ids = jnp.arange(NRES, dtype=jnp.int32)
    blk_ids = jnp.arange(LB, dtype=jnp.int32)
    small_cos, small_sin = dft_pair(res_ids, res_ids, NRES, 1.0 / math.sqrt(NRES))
    small_cos = small_cos.astype(jnp.bfloat16).astype(jnp.float32)
    small_sin = small_sin.astype(jnp.bfloat16).astype(jnp.float32)
    big_cos, big_sin = dft_pair(blk_ids, blk_ids, LB, 1.0 / math.sqrt(LB))
    big_cos = big_cos.astype(jnp.bfloat16).astype(jnp.float32)
    big_sin = big_sin.astype(jnp.bfloat16).astype(jnp.float32)
    twid_cos, twid_sin = dft_pair(res_ids, blk_ids, L, 1.0)
    high = lax.Precision.HIGHEST

    def one_window(window):
        extended = jnp.concatenate([window, jnp.zeros((2, K), jnp.bfloat16)], axis=1)
        wide = extended.astype(jnp.float32)[:, None, :]
        outcome = lax.conv_general_dilated(wide, filters, (1,), 'VALID', dimension_numbers=('CNH', 'OIH', 'CNH'), precision=high, preferred_element_type=jnp.float32)
        spectra = outcome[:, 0, :L].reshape(2, K, L)
        centered = wide[:, 0, K // 2:K // 2 + L]
        real_part = spectra[0] * centered[0][None, :] + spectra[1] * centered[1][None, :]
        imag_part = spectra[1] * centered[0][None, :] - spectra[0] * centered[1][None, :]
        products = jnp.stack([real_part, imag_part]).astype(jnp.bfloat16)
        products = lax.optimization_barrier(products).astype(jnp.float32).reshape(2, K, NRES, LB)
        section_real = jnp.einsum('qn,knm->kqm', small_cos, products[0], precision=high) + jnp.einsum('qn,knm->kqm', small_sin, products[1], precision=high)
        section_imag = jnp.einsum('qn,knm->kqm', small_cos, products[1], precision=high) - jnp.einsum('qn,knm->kqm', small_sin, products[0], precision=high)
        turned_real = section_real * twid_cos[None] + section_imag * twid_sin[None]
        turned_imag = section_imag * twid_cos[None] - section_real * twid_sin[None]
        partial_sums = jnp.stack([turned_real, turned_imag]).astype(jnp.bfloat16)
        partial_sums = lax.optimization_barrier(partial_sums).astype(jnp.float32)
        out_real = jnp.dot(partial_sums[0], big_cos, precision=high) + jnp.dot(partial_sums[1], big_sin, precision=high)
        out_imag = jnp.dot(partial_sums[1], big_cos, precision=high) - jnp.dot(partial_sums[0], big_sin, precision=high)
        return jnp.stack([out_real, out_imag]).astype(jnp.bfloat16)
    spectra_all = lax.map(one_window, jnp.transpose(signal, (1, 0, 2)))
    return jnp.transpose(spectra_all, (1, 2, 0, 3, 4))
```

```python
import functools
import math

import jax
import jax.numpy as jnp
import numpy as np
from jax import lax
from jax.experimental import pallas as pl
from jax.experimental.pallas import tpu as pltpu
from jax.sharding import PartitionSpec as P

K = 256
J = 256
HALF = 128
ALT = 64
TWO_PI = 2.0 * math.pi


def pair(phases, modulus):
    angles = TWO_PI * (phases % modulus) / modulus
    return np.cos(angles), np.sin(angles)


def small_dft(values):
    count = len(values)
    if count == 1:
        return values
    even = small_dft(values[0::2])
    odd = small_dft(values[1::2])
    low, high = [], []
    for i in range(count // 2):
        er, ei = even[i]
        orr, oi = odd[i]
        if i == 0:
            tr, ti = orr, oi
        elif 4 * i == count:
            tr, ti = oi, -orr
        else:
            c = math.cos(TWO_PI * i / count)
            s = math.sin(TWO_PI * i / count)
            if abs(c - s) < 1e-6:
                tr, ti = (orr + oi) * c, (oi - orr) * c
            elif abs(c + s) < 1e-6:
                tr, ti = (oi - orr) * s, (orr + oi) * (-s)
            else:
                tr, ti = orr * c + oi * s, oi * c - orr * s
        low.append((er + tr, ei + ti))
        high.append((er - tr, ei - ti))
    return low + high


def tables(blocks, block_len):
    d = block_len // J
    slots = J // (2 * blocks)
    total = blocks * block_len
    scale = 1.0 / math.sqrt(total * K)
    order = (
        HALF * d * np.arange(2)[:, None, None]
        + np.arange(d)[None, :, None]
        + d * np.arange(HALF)[None, None, :]
    ).reshape(-1)
    residues = np.arange(blocks)
    c, s = pair(residues[:, None] * order[None, :], total)
    lanes = np.stack([c, -s], axis=1) * scale
    c, s = pair(residues[:, None] * residues[None, :], blocks)
    folds = np.stack([c, -s], axis=1)[..., None] * np.ones(128)
    lane = np.arange(J)
    slot_of = (lane % HALF) // blocks
    slot = (np.arange(J) // (2 * blocks))[:, None] == slot_of[None, :]
    j = np.arange(HALF)
    b = d * j[None, :] + np.arange(d)[:, None]
    row = np.arange(J)
    lag = (row[None, :, None] - b[:, None, :]) % K
    start = ALT * (j // blocks)
    inside = (row[:, None] - start[None, :]) % K
    late = inside[None] < (b - start[None, :])[:, None, :]
    weight = 0.54 - 0.46 * np.cos(TWO_PI * lag / K)
    weight = np.where(late, -weight, weight)
    chan = np.arange(K)
    c, s = pair(chan[:, None] * row[None, :], K)
    emat = np.stack([np.concatenate([c, s], 1), np.concatenate([-s, c], 1)])
    c, s = pair(chan[:, None] * (d * j)[None, :], K)
    c1, s1 = pair(chan[:, None] * np.ones((1, HALF), np.int64), K)
    phase = np.stack([c, s, c1, s1])
    c, s = pair(row[:, None] * row[None, :], J)
    dft = np.concatenate([np.concatenate([c, -s], 1), np.concatenate([s, c], 1)], 0)
    twid = np.stack(pair(np.arange(d)[:, None] * row[None, :], block_len))
    f32 = lambda v: np.asarray(v, np.float32)
    b16 = lambda v: np.asarray(np.asarray(v, np.float32), jnp.bfloat16)
    return dict(
        lanes=f32(lanes), folds=f32(folds), slot=b16(slot), weight=f32(weight),
        emat=b16(emat), phase=f32(phase), dft=b16(dft), twid=f32(twid),
    )


def main_body(windows, blocks, block_len, chan, group):
    d = block_len // J
    ca = 2 * blocks
    slots = J // ca
    halves = block_len // 2
    rows = group * windows

    def body(
        xn_ref, zs_ref, slot_ref, weight_ref, dft_ref, twid_ref,
        lanes_hbm, folds_hbm, emat_hbm, phase_hbm, out_hbm,
        lanes_ref, folds_ref, emat_ref, phase_ref, turn_ref, spin_ref,
        lhs_ref, g_ref, out_ref, load_sem, out_sem,
    ):
        p = lax.axis_index("tm")
        s = lax.axis_index("strip")
        loads = [
            pltpu.make_async_copy(lanes_hbm.at[p], lanes_ref, load_sem.at[0]),
            pltpu.make_async_copy(folds_hbm.at[p], folds_ref, load_sem.at[1]),
            pltpu.make_async_copy(emat_hbm.at[:, pl.ds(s * chan, chan)], emat_ref, load_sem.at[2]),
            pltpu.make_async_copy(phase_hbm.at[:, pl.ds(s * chan, chan)], phase_ref, load_sem.at[3]),
        ]
        for load in loads:
            load.start()
        for load in loads:
            load.wait()
        br, bi = lanes_ref[0:1], lanes_ref[1:2]
        for q in range(block_len // 128):
            at = slice(q * 128, (q + 1) * 128)
            fr, fi = folds_ref[0], folds_ref[1]
            turn_ref[0, :, at] = fr * br[:, at] - fi * bi[:, at]
            turn_ref[1, :, at] = fr * bi[:, at] + fi * br[:, at]
        gr, gi = phase_ref[0], phase_ref[1]
        for o in range(d):
            if o > 0:
                gr, gi = gr * phase_ref[2] - gi * phase_ref[3], gr * phase_ref[3] + gi * phase_ref[2]
            spin_ref[o, 0] = gr
            spin_ref[o, 1] = gi

        low = lax.broadcasted_iota(jnp.int32, (ca, HALF), 1) < ALT
        emat = emat_ref[...].reshape(2 * chan, 2 * J)

        @pl.loop(0, windows)
        def _(w):
            def lane_tile(v):
                return xn_ref[w, :, v * 128 : (v + 1) * 128].astype(jnp.float32)

            for h in range(2):
                left, right, late = [], [], []
                for slot in range(slots):
                    g = (HALF * d * h) // ALT + slot
                    picks = []
                    for c in range(4):
                        n = g + (c - g) % 4
                        picks.append(n // 2)
                    for side, dst in ((0, left), (1, right)):
                        v0, v1 = picks[2 * side], picks[2 * side + 1]
                        x0 = lane_tile(v0)
                        dst.append(x0 if v0 == v1 else jnp.where(low, x0, lane_tile(v1)))
                    n = g + 4
                    tail = lane_tile(n // 2)
                    if n % 2:
                        tail = pltpu.roll(tail, ALT, 1)
                    late.append(-tail)
                lhs_ref[h, 0:ALT] = jnp.concatenate(late, axis=0).T[:ALT].astype(jnp.bfloat16)
                lhs_ref[h, ALT : ALT + HALF] = jnp.concatenate(left, axis=0).T.astype(jnp.bfloat16)
                lhs_ref[h, ALT + HALF :] = jnp.concatenate(right, axis=0).T.astype(jnp.bfloat16)

            for h in range(2):
                for o in range(0, d, 2):
                    at = slice(h * halves + o * HALF, h * halves + (o + 2) * HALF)
                    xs = zs_ref[w, :, at].astype(jnp.float32)
                    xr, xi = xs[:blocks], xs[blocks:]
                    er, ei = turn_ref[0, :, at], turn_ref[1, :, at]
                    zr = xr * er + xi * ei
                    zi = xr * ei - xi * er
                    mask = slot_ref[...]
                    zre = jnp.concatenate([zr, -zi], axis=0).astype(jnp.bfloat16)
                    zim = jnp.concatenate([zi, zr], axis=0).astype(jnp.bfloat16)
                    rhs = jnp.concatenate(
                        [
                            jnp.concatenate([zre] * slots, axis=0) * mask,
                            jnp.concatenate([zim] * slots, axis=0) * mask,
                        ],
                        axis=1,
                    )
                    lags = jnp.dot(lhs_ref[h], rhs, preferred_element_type=jnp.float32)
                    cols = []
                    for c in range(2):
                        for oo in range(2):
                            lanes = slice(c * J + oo * HALF, c * J + (oo + 1) * HALF)
                            late = lags[:ALT, lanes]
                            parts = []
                            for q in range(4):
                                t = weight_ref[o + oo, q * ALT : (q + 1) * ALT]
                                early = lags[(q + 1) * ALT : (q + 2) * ALT, lanes]
                                parts.append((jnp.where(t > 0, early, late) * t).astype(jnp.bfloat16))
                            cols.append(jnp.concatenate(parts, axis=0))
                    taps = jnp.concatenate(
                        [jnp.concatenate(cols[:2], axis=1), jnp.concatenate(cols[2:], axis=1)], axis=0
                    )
                    y = jnp.dot(emat, taps, preferred_element_type=jnp.float32)
                    for oo in range(2):
                        lanes = slice(oo * HALF, (oo + 1) * HALF)
                        yr, yi = y[:chan, lanes], y[chan:, lanes]
                        c, sn = spin_ref[o + oo, 0], spin_ref[o + oo, 1]
                        g_ref[o + oo, h, pl.ds(w, chan, stride=windows), :] = yr * c - yi * sn
                        g_ref[o + oo, 2 + h, pl.ds(w, chan, stride=windows), :] = yr * sn + yi * c

        chunks = chan // group

        def write(i, slot):
            return pltpu.make_async_copy(
                out_ref.at[slot], out_hbm.at[:, pl.ds(i * group, group)], out_sem.at[slot]
            )

        step = min(2, group)

        @pl.loop(0, chunks)
        def _(i):
            slot = lax.rem(i, 2)

            @pl.when(i >= 2)
            def _():
                write(i - 2, slot).wait()

            for u in range(0, group, step):
                first = i * rows + u * windows
                count = step * windows
                lhs = jnp.concatenate(
                    [
                        jnp.concatenate(
                            [g_ref[o, e, pl.ds(first, count), :].astype(jnp.bfloat16) for e in range(4)],
                            axis=1,
                        )
                        for o in range(d)
                    ],
                    axis=0,
                )
                inner = jnp.dot(lhs, dft_ref[...], preferred_element_type=jnp.float32)
                turned = []
                for o in range(d):
                    vr = inner[o * count : (o + 1) * count, :J]
                    vi = inner[o * count : (o + 1) * count, J:]
                    if o > 0:
                        tc, ts = twid_ref[0, o : o + 1], twid_ref[1, o : o + 1]
                        vr, vi = vr * tc + vi * ts, vi * tc - vr * ts
                    turned.append((vr, vi))
                for m, (yr, yi) in enumerate(small_dft(turned)):
                    lanes = slice(m * J, (m + 1) * J)
                    out_ref[slot, 0, u : u + step, :, lanes] = yr.astype(jnp.bfloat16).reshape(step, windows, J)
                    out_ref[slot, 1, u : u + step, :, lanes] = yi.astype(jnp.bfloat16).reshape(step, windows, J)
            write(i, slot).start()

        for i in range(max(chunks - 2, 0), chunks):
            write(i, i % 2).wait()

    return body


def gather_body(names, strips, blocks):
    count = strips * blocks

    def body(local_ref, every_ref, local_sem, send_sem, recv_sem):
        strip = lax.axis_index("strip")
        block = lax.axis_index("tm")
        me = strip * blocks + block

        def peer(step):
            other = lax.rem(me + step, count)
            where = {"strip": lax.div(other, blocks), "tm": lax.rem(other, blocks)}
            return tuple(where[name] for name in names)

        barrier = pltpu.get_barrier_semaphore()
        for step in range(1, count):
            pl.semaphore_signal(
                barrier, inc=1, device_id=peer(step), device_id_type=pl.DeviceIdType.MESH
            )
        own = pltpu.make_async_copy(local_ref, every_ref.at[strip, block], local_sem)
        own.start()
        pl.semaphore_wait(barrier, count - 1)
        copies = []
        for step in range(1, count):
            copy = pltpu.make_async_remote_copy(
                src_ref=local_ref,
                dst_ref=every_ref.at[strip, block],
                send_sem=send_sem.at[step - 1],
                recv_sem=recv_sem.at[step - 1],
                device_id=peer(step),
                device_id_type=pl.DeviceIdType.MESH,
            )
            copy.start()
            copies.append(copy)
        own.wait()
        for copy in copies:
            copy.wait()

    return body


def gather_everywhere(local, names, strips, blocks):
    return pl.pallas_call(
        gather_body(names, strips, blocks),
        out_shape=jax.ShapeDtypeStruct((strips, blocks) + local.shape, local.dtype),
        in_specs=[pl.BlockSpec(memory_space=pltpu.VMEM)],
        out_specs=pl.BlockSpec(memory_space=pl.ANY),
        scratch_shapes=[pltpu.SemaphoreType.DMA] + [pltpu.SemaphoreType.DMA((strips * blocks - 1,))] * 2,
        compiler_params=pltpu.CompilerParams(collective_id=0, has_side_effects=True),
        name="gather_everywhere",
    )(local)


def per_device(names, signal):
    blocks = lax.axis_size("tm")
    strips = lax.axis_size("strip")
    wloc, block_len = signal.shape[1], signal.shape[2]
    windows = wloc * strips
    chan = K // strips
    d = block_len // J
    ca = 2 * blocks
    tab = tables(blocks, block_len)

    every = gather_everywhere(signal.reshape(2 * wloc, block_len), names, strips, blocks)
    x = every.reshape(strips, blocks, 2, wloc, block_len).transpose(0, 3, 2, 1, 4)
    x = x.reshape(windows, 2, blocks, block_len)
    halo = jnp.concatenate([x[:, :, 1:, :K], jnp.zeros((windows, 2, 1, K), x.dtype)], axis=2)
    xn = jnp.concatenate([x, halo], axis=3).reshape(windows, ca, block_len + K)
    zs = xn[:, :, K // 2 : K // 2 + block_len].reshape(windows, ca, 2, HALF, d)
    zs = zs.transpose(0, 1, 2, 4, 3).reshape(windows, ca, block_len)

    group = min(8, chan)
    vmem = pl.BlockSpec(memory_space=pltpu.VMEM)
    hbm = pl.BlockSpec(memory_space=pl.ANY)
    out = pl.pallas_call(
        main_body(windows, blocks, block_len, chan, group),
        in_specs=[vmem] * 6 + [hbm] * 4,
        out_specs=hbm,
        out_shape=jax.ShapeDtypeStruct((2, chan, windows, block_len), jnp.bfloat16),
        scratch_shapes=[
            pltpu.VMEM((2, block_len), jnp.float32),
            pltpu.VMEM((2, blocks, 128), jnp.float32),
            pltpu.VMEM((2, chan, 2 * J), jnp.bfloat16),
            pltpu.VMEM((4, chan, HALF), jnp.float32),
            pltpu.VMEM((2, blocks, block_len), jnp.float32),
            pltpu.VMEM((d, 2, chan, HALF), jnp.float32),
            pltpu.VMEM((2, ALT + J, J), jnp.bfloat16),
            pltpu.VMEM((d, 4, chan * windows, HALF), jnp.float32),
            pltpu.VMEM((2, 2, group, windows, block_len), jnp.bfloat16),
            pltpu.SemaphoreType.DMA((4,)),
            pltpu.SemaphoreType.DMA((2,)),
        ],
        compiler_params=pltpu.CompilerParams(vmem_limit_bytes=56 * 1024 * 1024),
        name="strip_windows",
    )(xn, zs, tab["slot"], tab["weight"], tab["dft"], tab["twid"],
      tab["lanes"], tab["folds"], tab["emat"], tab["phase"])
    return out.reshape(2, chan, windows, 1, block_len)


def solution(mesh):
    return jax.shard_map(
        functools.partial(per_device, tuple(mesh.axis_names)),
        mesh=mesh,
        in_specs=(P(None, "strip", "tm"),),
        out_specs=P(None, "strip", None, "tm", None),
        check_vma=False,
    )
```

```python
import functools
import math

import jax
import jax.numpy as jnp
import numpy as np
from jax import lax
from jax.experimental import pallas as pl
from jax.experimental.pallas import tpu as pltpu
from jax.sharding import PartitionSpec as P

K = 256
J = 256
HALF = 128
ALT = 64
UNROLL = 2
TWO_PI = 2.0 * math.pi


def pair(phases, modulus):
    angles = TWO_PI * (phases % modulus) / modulus
    return np.cos(angles), np.sin(angles)


def small_dft(values):
    count = len(values)
    if count == 1:
        return values
    even = small_dft(values[0::2])
    odd = small_dft(values[1::2])
    low, high = [], []
    for i in range(count // 2):
        er, ei = even[i]
        orr, oi = odd[i]
        if i == 0:
            tr, ti = orr, oi
        elif 4 * i == count:
            tr, ti = oi, -orr
        else:
            c = math.cos(TWO_PI * i / count)
            s = math.sin(TWO_PI * i / count)
            if abs(c - s) < 1e-6:
                tr, ti = (orr + oi) * c, (oi - orr) * c
            elif abs(c + s) < 1e-6:
                tr, ti = (oi - orr) * s, (orr + oi) * (-s)
            else:
                tr, ti = orr * c + oi * s, oi * c - orr * s
        low.append((er + tr, ei + ti))
        high.append((er - tr, ei - ti))
    return low + high


def tables(blocks, block_len):
    d = block_len // J
    slots = J // (2 * blocks)
    total = blocks * block_len
    scale = 1.0 / math.sqrt(total * K)
    order = (
        HALF * d * np.arange(2)[:, None, None]
        + np.arange(d)[None, :, None]
        + d * np.arange(HALF)[None, None, :]
    ).reshape(-1)
    residues = np.arange(blocks)
    c, s = pair(residues[:, None] * order[None, :], total)
    lanes = np.stack([c, -s], axis=1) * scale
    c, s = pair(residues[:, None] * residues[None, :], blocks)
    folds = np.stack([c, -s], axis=1)[..., None] * np.ones(128)
    lane = np.arange(J)
    slot_of = (lane % HALF) // blocks
    slot = (np.arange(J) // (2 * blocks))[:, None] == slot_of[None, :]
    j = np.arange(HALF)
    b = d * j[None, :] + np.arange(d)[:, None]
    row = np.arange(J)
    lag = (row[None, :, None] - b[:, None, :]) % K
    start = ALT * (j // blocks)
    inside = (row[:, None] - start[None, :]) % K
    late = inside[None] < (b - start[None, :])[:, None, :]
    weight = 0.54 - 0.46 * np.cos(TWO_PI * lag / K)
    weight = np.where(late, -weight, weight)
    chan = np.arange(K)
    c, s = pair(chan[:, None] * row[None, :], K)
    emat = np.stack([np.concatenate([c, s], 1), np.concatenate([-s, c], 1)])
    c, s = pair(chan[:, None] * (d * j)[None, :], K)
    c1, s1 = pair(chan[:, None] * np.ones((1, HALF), np.int64), K)
    phase = np.stack([c, s, c1, s1])
    c, s = pair(row[:, None] * row[None, :], J)
    dft = np.concatenate([np.concatenate([c, -s], 1), np.concatenate([s, c], 1)], 0)
    twid = np.stack(pair(np.arange(d)[:, None] * row[None, :], block_len))
    f32 = lambda v: np.asarray(v, np.float32)
    b16 = lambda v: np.asarray(np.asarray(v, np.float32), jnp.bfloat16)
    return dict(
        lanes=f32(lanes), folds=f32(folds), slot=b16(slot), weight=f32(weight),
        emat=b16(emat), phase=f32(phase), dft=b16(dft), twid=f32(twid),
    )


def main_body(windows, blocks, block_len, chan, group):
    d = block_len // J
    ca = 2 * blocks
    slots = J // ca
    halves = block_len // 2
    pitch = windows + 1

    def body(
        xn_ref, zs_ref, slot_ref, weight_ref, dft_ref, twid_ref,
        lanes_hbm, folds_hbm, emat_hbm, phase_hbm, out_hbm,
        lanes_ref, folds_ref, emat_ref, phase_ref, turn_ref, spin_ref,
        lhs_ref, g_ref, out_ref, load_sem, out_sem,
    ):
        p = lax.axis_index("tm")
        s = lax.axis_index("strip")
        loads = [
            pltpu.make_async_copy(lanes_hbm.at[p], lanes_ref, load_sem.at[0]),
            pltpu.make_async_copy(folds_hbm.at[p], folds_ref, load_sem.at[1]),
            pltpu.make_async_copy(emat_hbm.at[:, pl.ds(s * chan, chan)], emat_ref, load_sem.at[2]),
            pltpu.make_async_copy(phase_hbm.at[:, pl.ds(s * chan, chan)], phase_ref, load_sem.at[3]),
        ]
        for load in loads:
            load.start()
        for load in loads:
            load.wait()
        br, bi = lanes_ref[0:1], lanes_ref[1:2]
        for q in range(block_len // 128):
            at = slice(q * 128, (q + 1) * 128)
            fr, fi = folds_ref[0], folds_ref[1]
            turn_ref[0, :, at] = fr * br[:, at] - fi * bi[:, at]
            turn_ref[1, :, at] = fr * bi[:, at] + fi * br[:, at]
        gr, gi = phase_ref[0], phase_ref[1]
        for o in range(d):
            if o > 0:
                gr, gi = gr * phase_ref[2] - gi * phase_ref[3], gr * phase_ref[3] + gi * phase_ref[2]
            spin_ref[o, 0] = gr
            spin_ref[o, 1] = gi

        low = lax.broadcasted_iota(jnp.int32, (ca, HALF), 1) < ALT
        emat = emat_ref[...].reshape(2 * chan, 2 * J)

        def build(w, slot):
            def lane_tile(v):
                return xn_ref[w, :, v * 128 : (v + 1) * 128].astype(jnp.float32)

            for h in range(2):
                left, right, late = [], [], []
                for part in range(slots):
                    g = (HALF * d * h) // ALT + part
                    picks = [(g + (c - g) % 4) // 2 for c in range(4)]
                    for side, dst in ((0, left), (1, right)):
                        v0, v1 = picks[2 * side], picks[2 * side + 1]
                        x0 = lane_tile(v0)
                        dst.append(x0 if v0 == v1 else jnp.where(low, x0, lane_tile(v1)))
                    n = g + 4
                    tail = lane_tile(n // 2)
                    if n % 2:
                        tail = pltpu.roll(tail, ALT, 1)
                    late.append(-tail)
                lhs_ref[slot, h, 0:ALT] = jnp.concatenate(late, axis=0).T[:ALT].astype(jnp.bfloat16)
                lhs_ref[slot, h, ALT : ALT + HALF] = jnp.concatenate(left, axis=0).T.astype(jnp.bfloat16)
                lhs_ref[slot, h, ALT + HALF :] = jnp.concatenate(right, axis=0).T.astype(jnp.bfloat16)

        def lag_products(w, slot, h, o):
            at = slice(h * halves + o * HALF, h * halves + (o + 2) * HALF)
            xs = zs_ref[w, :, at].astype(jnp.float32)
            xr, xi = xs[:blocks], xs[blocks:]
            er, ei = turn_ref[0, :, at], turn_ref[1, :, at]
            zr = xr * er + xi * ei
            zi = xr * ei - xi * er
            mask = slot_ref[...]
            zre = jnp.concatenate([zr, -zi], axis=0).astype(jnp.bfloat16)
            zim = jnp.concatenate([zi, zr], axis=0).astype(jnp.bfloat16)
            rhs = jnp.concatenate(
                [
                    jnp.concatenate([zre] * slots, axis=0) * mask,
                    jnp.concatenate([zim] * slots, axis=0) * mask,
                ],
                axis=1,
            )
            return jnp.dot(lhs_ref[slot, h], rhs, preferred_element_type=jnp.float32)

        def channels(w, h, o, lags):
            cols = []
            for c in range(2):
                for oo in range(2):
                    lanes = slice(c * J + oo * HALF, c * J + (oo + 1) * HALF)
                    late = lags[:ALT, lanes]
                    parts = []
                    for q in range(4):
                        t = weight_ref[o + oo, q * ALT : (q + 1) * ALT]
                        early = lags[(q + 1) * ALT : (q + 2) * ALT, lanes]
                        parts.append((jnp.where(t > 0, early, late) * t).astype(jnp.bfloat16))
                    cols.append(jnp.concatenate(parts, axis=0))
            taps = jnp.concatenate(
                [jnp.concatenate(cols[:2], axis=1), jnp.concatenate(cols[2:], axis=1)], axis=0
            )
            y = jnp.dot(emat, taps, preferred_element_type=jnp.float32)
            for oo in range(2):
                lanes = slice(oo * HALF, (oo + 1) * HALF)
                yr, yi = y[:chan, lanes], y[chan:, lanes]
                c, sn = spin_ref[o + oo, 0], spin_ref[o + oo, 1]
                g_ref[o + oo, h, pl.ds(w, chan, stride=pitch), :] = yr * c - yi * sn
                g_ref[o + oo, 2 + h, pl.ds(w, chan, stride=pitch), :] = yr * sn + yi * c

        build(0, 0)

        @pl.loop(0, windows // UNROLL)
        def _(i):
            pending = None
            for u in range(UNROLL):
                w = i * UNROLL + u
                build(jnp.minimum(w + 1, windows - 1), (u + 1) % 2)
                for h in range(2):
                    for o in range(0, d, 2):
                        lags = lag_products(w, u % 2, h, o)
                        if pending is not None:
                            channels(*pending)
                        pending = (w, h, o, lags)
            channels(*pending)

        chunks = chan // group

        def write(i, slot):
            return pltpu.make_async_copy(
                out_ref.at[slot], out_hbm.at[:, pl.ds(i * group, group)], out_sem.at[slot]
            )

        step = min(2, group)

        @pl.loop(0, chunks)
        def _(i):
            slot = lax.rem(i, 2)

            @pl.when(i >= 2)
            def _():
                write(i - 2, slot).wait()

            for u in range(0, group, step):
                count = step * windows
                lhs = jnp.concatenate(
                    [
                        jnp.concatenate(
                            [
                                g_ref[o, e, pl.ds((i * group + u + k) * pitch, windows), :].astype(jnp.bfloat16)
                                for e in range(4)
                            ],
                            axis=1,
                        )
                        for o in range(d)
                        for k in range(step)
                    ],
                    axis=0,
                )
                inner = jnp.dot(lhs, dft_ref[...], preferred_element_type=jnp.float32)
                turned = []
                for o in range(d):
                    vr = inner[o * count : (o + 1) * count, :J]
                    vi = inner[o * count : (o + 1) * count, J:]
                    if o > 0:
                        tc, ts = twid_ref[0, o : o + 1], twid_ref[1, o : o + 1]
                        vr, vi = vr * tc + vi * ts, vi * tc - vr * ts
                    turned.append((vr, vi))
                for m, (yr, yi) in enumerate(small_dft(turned)):
                    lanes = slice(m * J, (m + 1) * J)
                    out_ref[slot, 0, u : u + step, :, lanes] = yr.astype(jnp.bfloat16).reshape(step, windows, J)
                    out_ref[slot, 1, u : u + step, :, lanes] = yi.astype(jnp.bfloat16).reshape(step, windows, J)
            write(i, slot).start()

        for i in range(max(chunks - 2, 0), chunks):
            write(i, i % 2).wait()

    return body


def gather_body(names, strips, blocks, wloc, block_len):
    d = block_len // J
    ca = 2 * blocks
    pairs = blocks // 2
    lanes_o = J // d
    copies_sent = strips * blocks - 1

    def body(
        local_ref, rows_ref, lane_ref, xn_hbm, zs_hbm,
        every_ref, xn_ref, zs_ref, own_sem, send_sem, recv_sem, store_sem,
    ):
        s = lax.axis_index("strip")
        t = lax.axis_index("tm")
        other = t + 1 - 2 * lax.rem(t, 2)

        def device(strip, tm):
            where = {"strip": strip, "tm": tm}
            return tuple(where[name] for name in names)

        def strip_at(ds):
            return lax.rem(s + strips - ds, strips)

        def mate(dt):
            return lax.rem(t + blocks - 2 * dt, blocks)

        def rival(dt):
            return lax.rem(other + blocks - 2 * dt, blocks)

        across = [device(strip_at(strips - ds), t) for ds in range(1, strips)]
        inside = [device(s, mate(dt)) for dt in range(1, pairs)] + [device(s, other)]
        barrier = pltpu.get_barrier_semaphore()
        for peer in across + inside:
            pl.semaphore_signal(barrier, inc=1, device_id=peer, device_id_type=pl.DeviceIdType.MESH)
        own = pltpu.make_async_copy(local_ref, every_ref.at[s, t], own_sem)
        own.start()
        pl.semaphore_wait(barrier, len(across) + len(inside))

        sent = []

        def send(src, strip, tm, peer):
            copy = pltpu.make_async_remote_copy(
                src_ref=src,
                dst_ref=every_ref.at[strip, tm],
                send_sem=send_sem.at[len(sent)],
                recv_sem=recv_sem.at[strip, tm],
                device_id=peer,
                device_id_type=pl.DeviceIdType.MESH,
            )
            copy.start()
            sent.append(copy)

        def arrived(strip, tm):
            pltpu.make_async_remote_copy(
                src_ref=every_ref.at[strip, tm],
                dst_ref=every_ref.at[strip, tm],
                send_sem=send_sem.at[0],
                recv_sem=recv_sem.at[strip, tm],
                device_id=device(s, other),
                device_id_type=pl.DeviceIdType.MESH,
            ).wait_recv()

        for peer in across + inside:
            send(local_ref, s, t, peer)

        def relay(ds):
            arrived(strip_at(ds), t)
            for peer in inside:
                send(every_ref.at[strip_at(ds), t], strip_at(ds), t, peer)

        def hand_over(ds):
            for dt in range(1, pairs):
                arrived(strip_at(ds), mate(dt))
                send(every_ref.at[strip_at(ds), mate(dt)], strip_at(ds), mate(dt), device(s, other))

        def store(ds, which):
            at = pl.ds(strip_at(ds) * wloc, wloc)
            src, dst = ((xn_ref, xn_hbm), (zs_ref, zs_hbm))[which]
            return pltpu.make_async_copy(src.at[at], dst.at[at], store_sem.at[ds, which])

        def arrange(ds):
            for dt in range(pairs):
                arrived(strip_at(ds), rival(dt))
            first = strip_at(ds) * wloc
            slabs = [
                every_ref[strip_at(ds), a, c].astype(jnp.float32) for a in range(blocks) for c in range(2)
            ]
            flat = jnp.concatenate(slabs, axis=0).astype(jnp.bfloat16)
            count = ca * wloc
            nat = jnp.dot(rows_ref[0], flat, preferred_element_type=jnp.float32).astype(jnp.bfloat16)
            halo = jnp.dot(rows_ref[1], flat[:, :K], preferred_element_type=jnp.float32).astype(jnp.bfloat16)
            full = jnp.concatenate([nat, halo], axis=1)
            for wl in range(wloc):
                xn_ref[first + wl] = full[wl * ca : (wl + 1) * ca]
            moved = jnp.concatenate(
                [full[:, HALF + q * J : HALF + (q + 1) * J] for q in range(block_len // J)], axis=0
            )
            moved = jnp.dot(moved, lane_ref[...], preferred_element_type=jnp.float32)
            for h in range(2):
                for o in range(d):
                    lanes = slice(o * lanes_o, (o + 1) * lanes_o)
                    part = jnp.concatenate(
                        [
                            moved[q * count : (q + 1) * count, lanes]
                            for q in range(h * d // 2, (h + 1) * d // 2)
                        ],
                        axis=1,
                    ).astype(jnp.bfloat16)
                    for wl in range(wloc):
                        zs_ref[first + wl, :, (h * d + o) * HALF : (h * d + o + 1) * HALF] = part[
                            wl * ca : (wl + 1) * ca
                        ]
            store(ds, 0).start()
            store(ds, 1).start()

        near = [1, strips - 1] if strips > 2 else [1]
        far = [ds for ds in range(1, strips) if ds not in near]
        for ds in near:
            relay(ds)
        hand_over(0)
        for ds in far:
            relay(ds)
        own.wait()
        arrange(0)
        for ds in near + far:
            hand_over(ds)
            arrange(ds)
        for copy in sent:
            copy.wait_send()
        for ds in range(strips):
            store(ds, 0).wait()
            store(ds, 1).wait()

    return body


def gather_everywhere(signal, names, strips, blocks):
    wloc, block_len = signal.shape[1], signal.shape[2]
    d = block_len // J
    windows = wloc * strips
    ca = 2 * blocks
    count = ca * wloc
    lanes_o = J // d
    w, c, a = np.meshgrid(np.arange(wloc), np.arange(2), np.arange(blocks), indexing="ij")
    target = ((w * 2 + c) * blocks + a).reshape(-1)
    source = ((a * 2 + c) * wloc + w).reshape(-1)
    rows = np.zeros((2, count, count))
    rows[0, target, source] = 1.0
    inner = a.reshape(-1) + 1 < blocks
    rows[1, target[inner], source[inner] + 2 * wloc] = 1.0
    lane = np.zeros((J, J))
    n = np.arange(J)
    lane[n, (n % d) * lanes_o + n // d] = 1.0
    vmem = pl.BlockSpec(memory_space=pltpu.VMEM)
    hbm = pl.BlockSpec(memory_space=pl.ANY)
    xn = (windows, ca, block_len + K)
    zs = (windows, ca, block_len)
    return pl.pallas_call(
        gather_body(names, strips, blocks, wloc, block_len),
        out_shape=[jax.ShapeDtypeStruct(xn, signal.dtype), jax.ShapeDtypeStruct(zs, signal.dtype)],
        in_specs=[vmem] * 3,
        out_specs=[hbm] * 2,
        scratch_shapes=[
            pltpu.VMEM((strips, blocks, 2, wloc, block_len), signal.dtype),
            pltpu.VMEM(xn, signal.dtype),
            pltpu.VMEM(zs, signal.dtype),
            pltpu.SemaphoreType.DMA,
            pltpu.SemaphoreType.DMA((strips * blocks - 1,)),
            pltpu.SemaphoreType.DMA((strips, blocks)),
            pltpu.SemaphoreType.DMA((strips, 2)),
        ],
        compiler_params=pltpu.CompilerParams(collective_id=0, has_side_effects=True),
        name="gather_everywhere",
    )(signal, np.asarray(rows, jnp.bfloat16), np.asarray(lane, jnp.bfloat16))


def per_device(names, signal):
    blocks = lax.axis_size("tm")
    strips = lax.axis_size("strip")
    wloc, block_len = signal.shape[1], signal.shape[2]
    windows = wloc * strips
    chan = K // strips
    d = block_len // J
    ca = 2 * blocks
    tab = tables(blocks, block_len)

    xn, zs = gather_everywhere(signal, names, strips, blocks)
    group = min(8, chan)
    vmem = pl.BlockSpec(memory_space=pltpu.VMEM)
    hbm = pl.BlockSpec(memory_space=pl.ANY)
    out = pl.pallas_call(
        main_body(windows, blocks, block_len, chan, group),
        in_specs=[vmem] * 6 + [hbm] * 4,
        out_specs=hbm,
        out_shape=jax.ShapeDtypeStruct((2, chan, windows, block_len), jnp.bfloat16),
        scratch_shapes=[
            pltpu.VMEM((2, block_len), jnp.float32),
            pltpu.VMEM((2, blocks, 128), jnp.float32),
            pltpu.VMEM((2, chan, 2 * J), jnp.bfloat16),
            pltpu.VMEM((4, chan, HALF), jnp.float32),
            pltpu.VMEM((2, blocks, block_len), jnp.float32),
            pltpu.VMEM((d, 2, chan, HALF), jnp.float32),
            pltpu.VMEM((2, 2, ALT + J, J), jnp.bfloat16),
            pltpu.VMEM((d, 4, chan * (windows + 1), HALF), jnp.float32),
            pltpu.VMEM((2, 2, group, windows, block_len), jnp.bfloat16),
            pltpu.SemaphoreType.DMA((4,)),
            pltpu.SemaphoreType.DMA((2,)),
        ],
        compiler_params=pltpu.CompilerParams(vmem_limit_bytes=56 * 1024 * 1024),
        name="strip_windows",
    )(xn, zs, tab["slot"], tab["weight"], tab["dft"], tab["twid"],
      tab["lanes"], tab["folds"], tab["emat"], tab["phase"])
    return out.reshape(2, chan, windows, 1, block_len)


def solution(mesh):
    return jax.shard_map(
        functools.partial(per_device, tuple(mesh.axis_names)),
        mesh=mesh,
        in_specs=(P(None, "strip", "tm"),),
        out_specs=P(None, "strip", None, "tm", None),
        check_vma=False,
    )
```

```python
import functools
import math

import jax
import jax.numpy as jnp
import numpy as np
from jax import lax
from jax.experimental import pallas as pl
from jax.experimental.pallas import tpu as pltpu
from jax.sharding import PartitionSpec as P

K = 256
J = 256
HALF = 128
ALT = 64
UNROLL = 2
GROUP = 8
TWO_PI = 2.0 * math.pi


def pair(phases, modulus):
    angles = TWO_PI * (phases % modulus) / modulus
    return np.cos(angles), np.sin(angles)


def small_dft(values):
    count = len(values)
    if count == 1:
        return values
    even = small_dft(values[0::2])
    odd = small_dft(values[1::2])
    low, high = [], []
    for i in range(count // 2):
        er, ei = even[i]
        orr, oi = odd[i]
        if i == 0:
            tr, ti = orr, oi
        elif 4 * i == count:
            tr, ti = oi, -orr
        else:
            c = math.cos(TWO_PI * i / count)
            s = math.sin(TWO_PI * i / count)
            if abs(c - s) < 1e-6:
                tr, ti = (orr + oi) * c, (oi - orr) * c
            elif abs(c + s) < 1e-6:
                tr, ti = (oi - orr) * s, (orr + oi) * (-s)
            else:
                tr, ti = orr * c + oi * s, oi * c - orr * s
        low.append((er + tr, ei + ti))
        high.append((er - tr, ei - ti))
    return low + high


def tables(blocks, block_len):
    d = block_len // J
    slots = J // (2 * blocks)
    total = blocks * block_len
    scale = 1.0 / math.sqrt(total * K)
    order = (
        HALF * d * np.arange(2)[:, None, None]
        + np.arange(d)[None, :, None]
        + d * np.arange(HALF)[None, None, :]
    ).reshape(-1)
    residues = np.arange(blocks)
    c, s = pair(residues[:, None] * order[None, :], total)
    lanes = np.stack([c, -s], axis=1) * scale
    c, s = pair(residues[:, None] * residues[None, :], blocks)
    folds = np.stack([c, -s], axis=1)[..., None] * np.ones(128)
    lane = np.arange(J)
    slot_of = (lane % HALF) // blocks
    slot = (np.arange(J) // (2 * blocks))[:, None] == slot_of[None, :]
    j = np.arange(HALF)
    b = d * j[None, :] + np.arange(d)[:, None]
    row = np.arange(J)
    lag = (row[None, :, None] - b[:, None, :]) % K
    start = ALT * (j // blocks)
    inside = (row[:, None] - start[None, :]) % K
    late = inside[None] < (b - start[None, :])[:, None, :]
    weight = 0.54 - 0.46 * np.cos(TWO_PI * lag / K)
    weight = np.stack([np.where(late, 0.0, weight), np.where(late, -weight, 0.0)], axis=1)
    chan = np.arange(K)
    c, s = pair(chan[:, None] * row[None, :], K)
    emat = np.stack([np.concatenate([c, s], 1), np.concatenate([-s, c], 1)])
    c, s = pair(chan[:, None] * (d * j)[None, :], K)
    c1, s1 = pair(chan[:, None] * np.ones((1, HALF), np.int64), K)
    phase = np.stack([c, s, c1, s1])
    c, s = pair(row[:, None] * row[None, :], J)
    dft = np.concatenate([np.concatenate([c, -s], 1), np.concatenate([s, c], 1)], 0)
    twid = np.stack(pair(np.arange(d)[:, None] * row[None, :], block_len))
    f32 = lambda v: np.asarray(v, np.float32)
    b16 = lambda v: np.asarray(np.asarray(v, np.float32), jnp.bfloat16)
    return dict(
        lanes=f32(lanes), folds=f32(folds), slot=b16(slot), weight=b16(weight),
        emat=b16(emat), phase=f32(phase), dft=b16(dft), twid=f32(twid),
    )


def in_hbm(value):
    return pltpu.with_memory_space_constraint(jnp.asarray(value), pltpu.HBM)


def first_body(names, strips, blocks, wloc, block_len, chan):
    d = block_len // J
    ca = 2 * blocks
    slots = J // ca
    halves = block_len // 2
    pairs = blocks // 2
    lanes_o = J // d
    count = ca * wloc

    def body(
        local_hbm, rows_hbm, lane_hbm, slot_hbm,
        weight_hbm, lanes_hbm, folds_hbm, emat_hbm, phase_hbm, g_ref,
        local_ref, rows_ref, lane_ref, slot_ref,
        every_ref, next_xn_ref, next_zs_ref, xn_ref, zs_ref, lhs_ref,
        weight_ref, lanes_ref, folds_ref, emat_ref, phase_ref, turn_ref, spin_ref,
        load_sem, direct_sem, relay_sem, hand_sem, recv_sem,
    ):
        s = lax.axis_index("strip")
        t = lax.axis_index("tm")
        other = t + 1 - 2 * lax.rem(t, 2)

        def device(strip, tm):
            where = {"strip": strip, "tm": tm}
            return tuple(where[name] for name in names)

        def strip_at(ds):
            return lax.rem(s + strips - ds, strips)

        def mate(dt):
            return lax.rem(t + blocks - 2 * dt, blocks)

        def rival(dt):
            return lax.rem(other + blocks - 2 * dt, blocks)

        across = [device(strip_at(strips - ds), t) for ds in range(1, strips)]
        inside = [device(s, mate(dt)) for dt in range(1, pairs)] + [device(s, other)]
        barrier = pltpu.get_barrier_semaphore()
        for peer in across + inside:
            pl.semaphore_signal(barrier, inc=1, device_id=peer, device_id_type=pl.DeviceIdType.MESH)
        local = pltpu.make_async_copy(local_hbm, local_ref, load_sem.at[8])
        local.start()
        loads = [
            pltpu.make_async_copy(rows_hbm, rows_ref, load_sem.at[5]),
            pltpu.make_async_copy(lane_hbm, lane_ref, load_sem.at[6]),
            pltpu.make_async_copy(slot_hbm, slot_ref, load_sem.at[7]),
            pltpu.make_async_copy(lanes_hbm.at[t], lanes_ref, load_sem.at[0]),
            pltpu.make_async_copy(folds_hbm.at[t], folds_ref, load_sem.at[1]),
            pltpu.make_async_copy(emat_hbm.at[:, pl.ds(s * chan, chan)], emat_ref, load_sem.at[2]),
            pltpu.make_async_copy(phase_hbm.at[:, pl.ds(s * chan, chan)], phase_ref, load_sem.at[3]),
            pltpu.make_async_copy(weight_hbm, weight_ref, load_sem.at[4]),
        ]
        for load in loads:
            load.start()
        local.wait()
        every_ref[s, t] = jnp.concatenate(
            [local_ref[0].astype(jnp.float32), local_ref[1].astype(jnp.float32)], axis=0
        ).astype(jnp.bfloat16)
        pl.semaphore_wait(barrier, len(across) + len(inside))

        def transfer(strip, tm, peer, send_sem):
            return pltpu.make_async_remote_copy(
                src_ref=every_ref.at[strip, tm],
                dst_ref=every_ref.at[strip, tm],
                send_sem=send_sem,
                recv_sem=recv_sem.at[strip, tm],
                device_id=peer,
                device_id_type=pl.DeviceIdType.MESH,
            )

        def arrived(strip, tm):
            transfer(strip, tm, inside[-1], direct_sem.at[0]).wait_recv()

        def direct(i):
            return transfer(s, t, (across + inside)[i], direct_sem.at[i])

        def relay(ds, i):
            return transfer(strip_at(ds), t, inside[i], relay_sem.at[ds, i])

        def hand(ds, dt):
            return transfer(strip_at(ds), mate(dt), inside[-1], hand_sem.at[ds, dt])

        def relay_all(ds):
            arrived(strip_at(ds), t)
            for i in range(len(inside)):
                relay(ds, i).start()

        def hand_over(ds):
            for dt in range(1, pairs):
                arrived(strip_at(ds), mate(dt))
                hand(ds, dt).start()

        def complete(ds):
            for dt in range(pairs):
                arrived(strip_at(ds), rival(dt))

        for i in range(len(across) + len(inside)):
            direct(i).start()

        low = lax.broadcasted_iota(jnp.int32, (ca, HALF), 1) < ALT

        def rows_of(ds):
            flat = every_ref[strip_at(ds)].reshape(count, block_len)
            nat = jnp.dot(rows_ref[0], flat, preferred_element_type=jnp.float32).astype(jnp.bfloat16)
            halo = jnp.dot(rows_ref[1], flat[:, :K], preferred_element_type=jnp.float32).astype(jnp.bfloat16)
            for wl in range(wloc):
                next_xn_ref[wl, :, :block_len] = nat[wl * ca : (wl + 1) * ca]
                next_xn_ref[wl, :, block_len:] = halo[wl * ca : (wl + 1) * ca]
            return jnp.concatenate([nat[:, HALF:], halo[:, :HALF]], axis=1)

        def lanes_of(full):
            moved = jnp.concatenate([full[:, q * J : (q + 1) * J] for q in range(block_len // J)], axis=0)
            moved = jnp.dot(moved, lane_ref[...], preferred_element_type=jnp.float32)
            for h in range(2):
                for o in range(d):
                    lanes = slice(o * lanes_o, (o + 1) * lanes_o)
                    part = jnp.concatenate(
                        [
                            moved[q * count : (q + 1) * count, lanes]
                            for q in range(h * d // 2, (h + 1) * d // 2)
                        ],
                        axis=1,
                    ).astype(jnp.bfloat16)
                    for wl in range(wloc):
                        next_zs_ref[wl, :, (h * d + o) * HALF : (h * d + o + 1) * HALF] = part[
                            wl * ca : (wl + 1) * ca
                        ]

        def build(src_ref, wl, slot):
            def lane_tile(v):
                return src_ref[wl, :, v * 128 : (v + 1) * 128].astype(jnp.float32)

            for h in range(2):
                left, right, late = [], [], []
                for part in range(slots):
                    g = (HALF * d * h) // ALT + part
                    picks = [(g + (c - g) % 4) // 2 for c in range(4)]
                    for side, dst in ((0, left), (1, right)):
                        v0, v1 = picks[2 * side], picks[2 * side + 1]
                        x0 = lane_tile(v0)
                        dst.append(x0 if v0 == v1 else jnp.where(low, x0, lane_tile(v1)))
                    n = g + 4
                    tail = lane_tile(n // 2)
                    if n % 2:
                        tail = pltpu.roll(tail, ALT, 1)
                    late.append(-tail)
                lhs_ref[slot, h, 0:ALT] = jnp.concatenate(late, axis=0).T[:ALT].astype(jnp.bfloat16)
                lhs_ref[slot, h, ALT : ALT + HALF] = jnp.concatenate(left, axis=0).T.astype(jnp.bfloat16)
                lhs_ref[slot, h, ALT + HALF :] = jnp.concatenate(right, axis=0).T.astype(jnp.bfloat16)

        def lag_products(wl, h, o):
            at = slice(h * halves + o * HALF, h * halves + (o + 2) * HALF)
            xs = zs_ref[wl, :, at].astype(jnp.float32)
            xr, xi = xs[:blocks], xs[blocks:]
            er, ei = turn_ref[0, :, at], turn_ref[1, :, at]
            zr = xr * er + xi * ei
            zi = xr * ei - xi * er
            mask = slot_ref[...]
            zre = jnp.concatenate([zr, -zi], axis=0).astype(jnp.bfloat16)
            zim = jnp.concatenate([zi, zr], axis=0).astype(jnp.bfloat16)
            rhs = jnp.concatenate(
                [
                    jnp.concatenate([zre] * slots, axis=0) * mask,
                    jnp.concatenate([zim] * slots, axis=0) * mask,
                ],
                axis=1,
            )
            return jnp.dot(lhs_ref[wl % 2, h], rhs, preferred_element_type=jnp.float32)

        def channels(ds, wl, h, o, lags):
            w = strip_at(ds) * wloc + wl
            emat = emat_ref[...].reshape(2 * chan, 2 * J)
            cols = []
            for c in range(2):
                for oo in range(2):
                    lanes = slice(c * J + oo * HALF, c * J + (oo + 1) * HALF)
                    late = lags[:ALT, lanes].astype(jnp.bfloat16)
                    parts = []
                    for q in range(4):
                        at = slice(q * ALT, (q + 1) * ALT)
                        early = lags[(q + 1) * ALT : (q + 2) * ALT, lanes].astype(jnp.bfloat16)
                        parts.append(early * weight_ref[o + oo, 0, at] + late * weight_ref[o + oo, 1, at])
                    cols.append(jnp.concatenate(parts, axis=0))
            taps = jnp.concatenate(
                [jnp.concatenate(cols[:2], axis=1), jnp.concatenate(cols[2:], axis=1)], axis=0
            )
            y = jnp.dot(emat, taps, preferred_element_type=jnp.float32)
            for oo in range(2):
                lanes = slice(oo * HALF, (oo + 1) * HALF)
                yr, yi = y[:chan, lanes], y[chan:, lanes]
                c, sn = spin_ref[o + oo, 0], spin_ref[o + oo, 1]
                gr = (yr * c - yi * sn).astype(jnp.bfloat16).reshape(chan // GROUP, GROUP, HALF)
                gi = (yr * sn + yi * c).astype(jnp.bfloat16).reshape(chan // GROUP, GROUP, HALF)
                g_ref[:, w, o + oo, :, h * HALF : (h + 1) * HALF] = gr
                g_ref[:, w, o + oo, :, J + h * HALF : J + (h + 1) * HALF] = gi

        near = [1, strips - 1] if strips > 2 else [1]
        far = [ds for ds in range(1, strips) if ds not in near]
        for ds in near:
            relay_all(ds)
        hand_over(0)
        for ds in far:
            relay_all(ds)

        for load in loads:
            load.wait()
        br, bi = lanes_ref[0:1], lanes_ref[1:2]
        for q in range(block_len // 128):
            at = slice(q * 128, (q + 1) * 128)
            fr, fi = folds_ref[0], folds_ref[1]
            turn_ref[0, :, at] = fr * br[:, at] - fi * bi[:, at]
            turn_ref[1, :, at] = fr * bi[:, at] + fi * br[:, at]
        gr, gi = phase_ref[0], phase_ref[1]
        for o in range(d):
            if o > 0:
                gr, gi = gr * phase_ref[2] - gi * phase_ref[3], gr * phase_ref[3] + gi * phase_ref[2]
            spin_ref[o, 0] = gr
            spin_ref[o, 1] = gi

        complete(0)
        lanes_of(rows_of(0))
        build(next_xn_ref, 0, 0)

        @pl.loop(0, strips)
        def _(ds):
            xn_ref[...] = next_xn_ref[...]
            zs_ref[...] = next_zs_ref[...]
            after = jnp.minimum(ds + 1, strips - 1)

            @pl.when(ds + 1 < strips)
            def _():
                hand_over(ds + 1)

            for first in range(0, wloc, UNROLL):
                last = first + UNROLL >= wloc
                mine = range(first, min(first + UNROLL, wloc))

                if last:

                    @pl.when(ds + 1 < strips)
                    def _():
                        complete(ds + 1)

                    full = rows_of(after)
                pending = None
                for wl in mine:
                    if wl + 1 < wloc:
                        build(xn_ref, wl + 1, (wl + 1) % 2)
                    else:
                        build(next_xn_ref, 0, 0)
                    for h in range(2):
                        for o in range(0, d, 2):
                            lags = lag_products(wl, h, o)
                            if pending is not None:
                                channels(*pending)
                            pending = (ds, wl, h, o, lags)
                        if last and wl == first and h == 0:
                            lanes_of(full)
                channels(*pending)

        for i in range(len(across) + len(inside)):
            direct(i).wait_send()
        for ds in range(strips):
            if ds > 0:
                for i in range(len(inside)):
                    relay(ds, i).wait_send()
            for dt in range(1, pairs):
                hand(ds, dt).wait_send()

    return body


def arrangements(blocks, wloc, d):
    count = 2 * blocks * wloc
    w, c, a = np.meshgrid(np.arange(wloc), np.arange(2), np.arange(blocks), indexing="ij")
    target = ((w * 2 + c) * blocks + a).reshape(-1)
    source = ((a * 2 + c) * wloc + w).reshape(-1)
    rows = np.zeros((2, count, count))
    rows[0, target, source] = 1.0
    inner = a.reshape(-1) + 1 < blocks
    rows[1, target[inner], source[inner] + 2 * wloc] = 1.0
    lane = np.zeros((J, J))
    n = np.arange(J)
    lane[n, (n % d) * (J // d) + n // d] = 1.0
    return np.asarray(rows, jnp.bfloat16), np.asarray(lane, jnp.bfloat16)


def first_phase(signal, tab, names, strips, blocks):
    wloc, block_len = signal.shape[1], signal.shape[2]
    d = block_len // J
    chan = K // strips
    windows = wloc * strips
    ca = 2 * blocks
    rows, lane = arrangements(blocks, wloc, d)
    hbm = pl.BlockSpec(memory_space=pltpu.HBM)
    b16, f32 = jnp.bfloat16, jnp.float32
    peers = strips - 1 + blocks // 2
    return pl.pallas_call(
        first_body(names, strips, blocks, wloc, block_len, chan),
        out_shape=pltpu.VMEM((chan // GROUP, windows, d, GROUP, 2 * J), b16),
        in_specs=[hbm] * 9,
        out_specs=pl.BlockSpec(memory_space=pltpu.VMEM),
        scratch_shapes=[
            pltpu.VMEM((2, wloc, block_len), b16),
            pltpu.VMEM((2, ca * wloc, ca * wloc), b16),
            pltpu.VMEM((J, J), b16),
            pltpu.VMEM((J, J), b16),
            pltpu.VMEM((strips, blocks, 2 * wloc, block_len), b16),
            pltpu.VMEM((wloc, ca, block_len + K), b16),
            pltpu.VMEM((wloc, ca, block_len), b16),
            pltpu.VMEM((wloc, ca, block_len + K), b16),
            pltpu.VMEM((wloc, ca, block_len), b16),
            pltpu.VMEM((2, 2, ALT + J, J), b16),
            pltpu.VMEM((d, 2, J, HALF), b16),
            pltpu.VMEM((2, block_len), f32),
            pltpu.VMEM((2, blocks, 128), f32),
            pltpu.VMEM((2, chan, 2 * J), b16),
            pltpu.VMEM((4, chan, HALF), f32),
            pltpu.VMEM((2, blocks, block_len), f32),
            pltpu.VMEM((d, 2, chan, HALF), f32),
            pltpu.SemaphoreType.DMA((9,)),
            pltpu.SemaphoreType.DMA((peers,)),
            pltpu.SemaphoreType.DMA((strips, blocks // 2)),
            pltpu.SemaphoreType.DMA((strips, blocks // 2)),
            pltpu.SemaphoreType.DMA((strips, blocks)),
        ],
        compiler_params=pltpu.CompilerParams(
            collective_id=0, has_side_effects=True, vmem_limit_bytes=24 * 1024 * 1024
        ),
        name="lag_channels",
    )(*map(in_hbm, (signal, rows, lane, tab["slot"], tab["weight"], tab["lanes"], tab["folds"], tab["emat"], tab["phase"])))


def final_body(chunks, windows, block_len):
    d = block_len // J
    pitch = GROUP + 1
    step = 4
    span = 8
    unroll = 2 if chunks % 2 == 0 else 1

    def body(g_ref, dft_hbm, twid_hbm, out_hbm, dft_ref, twid_ref, out_ref, y_ref, table_sem, out_sem):
        def write(i):
            at = pl.ds(i * GROUP, GROUP)
            return pltpu.make_async_copy(out_ref.at[:, at], out_hbm.at[:, at], out_sem.at[i])

        tables_in = [
            pltpu.make_async_copy(dft_hbm, dft_ref, table_sem.at[0]),
            pltpu.make_async_copy(twid_hbm, twid_ref, table_sem.at[1]),
        ]
        for copy in tables_in:
            copy.start()
        for copy in tables_in:
            copy.wait()

        def windows_of(i, u, w0):
            count = step * GROUP
            lhs = jnp.concatenate(
                [g_ref[i, w0 : w0 + step, o].reshape(count, 2 * J) for o in range(d)], axis=0
            )
            inner = jnp.dot(lhs, dft_ref[...], preferred_element_type=jnp.float32)
            turned = []
            for o in range(d):
                vr = inner[o * count : (o + 1) * count, :J]
                vi = inner[o * count : (o + 1) * count, J:]
                if o > 0:
                    tc, ts = twid_ref[0, o : o + 1], twid_ref[1, o : o + 1]
                    vr, vi = vr * tc + vi * ts, vi * tc - vr * ts
                turned.append((vr, vi))
            for m, both in enumerate(small_dft(turned)):
                for c in range(2):
                    for q in range(J // 128):
                        for wi in range(step):
                            y_ref[u, c, m * (J // 128) + q, pl.ds((w0 + wi) * pitch, GROUP), :] = both[c][
                                wi * GROUP : (wi + 1) * GROUP, q * 128 : (q + 1) * 128
                            ]
            if (w0 + step) % span == 0:
                w1 = w0 + step - span
                for k in range(GROUP):
                    for c in range(2):
                        for q in range(block_len // 128):
                            out_ref[c, i * GROUP + k, w1 : w1 + span, q * 128 : (q + 1) * 128] = y_ref[
                                u, c, q, pl.ds(w1 * pitch + k, span, stride=pitch), :
                            ].astype(jnp.bfloat16)

        @pl.loop(0, chunks // unroll)
        def _(n):
            for u in range(unroll):
                for w0 in range(0, windows, step):
                    windows_of(n * unroll + u, u, w0)
            for u in range(unroll):
                write(n * unroll + u).start()

        @pl.loop(0, chunks)
        def _(i):
            write(i).wait()

    return body


def final_phase(g, tab):
    chunks, windows, d, _, wide = g.shape
    block_len = d * J
    chan = chunks * GROUP
    hbm = pl.BlockSpec(memory_space=pltpu.HBM)
    b16, f32 = jnp.bfloat16, jnp.float32
    return pl.pallas_call(
        final_body(chunks, windows, block_len),
        in_specs=[pl.BlockSpec(memory_space=pltpu.VMEM), hbm, hbm],
        out_specs=hbm,
        out_shape=jax.ShapeDtypeStruct((2, chan, windows, block_len), b16),
        scratch_shapes=[
            pltpu.VMEM((wide, wide), b16),
            pltpu.VMEM((2, d, J), f32),
            pltpu.VMEM((2, chan, windows, block_len), b16),
            pltpu.VMEM((2, 2, block_len // 128, windows * (GROUP + 1), 128), f32),
            pltpu.SemaphoreType.DMA((2,)),
            pltpu.SemaphoreType.DMA((chunks,)),
        ],
        compiler_params=pltpu.CompilerParams(vmem_limit_bytes=28 * 1024 * 1024),
        name="frequencies",
    )(pltpu.with_memory_space_constraint(g, pltpu.VMEM), in_hbm(tab["dft"]), in_hbm(tab["twid"]))


def per_device(names, signal):
    blocks = lax.axis_size("tm")
    strips = lax.axis_size("strip")
    wloc, block_len = signal.shape[1], signal.shape[2]
    tab = tables(blocks, block_len)
    g = first_phase(signal, tab, names, strips, blocks)
    out = final_phase(g, tab)
    return out.reshape(2, K // strips, wloc * strips, 1, block_len)


def solution(mesh):
    return jax.shard_map(
        functools.partial(per_device, tuple(mesh.axis_names)),
        mesh=mesh,
        in_specs=(P(None, "strip", "tm"),),
        out_specs=P(None, "strip", None, "tm", None),
        check_vma=False,
    )
```

```python
import functools
import math

import jax
import jax.numpy as jnp
import numpy as np
from jax import lax
from jax.experimental import pallas as pl
from jax.experimental.pallas import tpu as pltpu
from jax.sharding import PartitionSpec as P

K = 256
J = 256
HALF = 128
ALT = 64
UNROLL = 2
GROUP = 8
TWO_PI = 2.0 * math.pi


def pair(phases, modulus):
    angles = TWO_PI * (phases % modulus) / modulus
    return np.cos(angles), np.sin(angles)


def small_dft(values):
    count = len(values)
    if count == 1:
        return values
    even = small_dft(values[0::2])
    odd = small_dft(values[1::2])
    low, high = [], []
    for i in range(count // 2):
        er, ei = even[i]
        orr, oi = odd[i]
        if i == 0:
            tr, ti = orr, oi
        elif 4 * i == count:
            tr, ti = oi, -orr
        else:
            c = math.cos(TWO_PI * i / count)
            s = math.sin(TWO_PI * i / count)
            if abs(c - s) < 1e-6:
                tr, ti = (orr + oi) * c, (oi - orr) * c
            elif abs(c + s) < 1e-6:
                tr, ti = (oi - orr) * s, (orr + oi) * (-s)
            else:
                tr, ti = orr * c + oi * s, oi * c - orr * s
        low.append((er + tr, ei + ti))
        high.append((er - tr, ei - ti))
    return low + high


def tables(blocks, block_len):
    d = block_len // J
    slots = J // (2 * blocks)
    total = blocks * block_len
    scale = 1.0 / math.sqrt(total * K)
    order = (
        HALF * d * np.arange(2)[:, None, None]
        + np.arange(d)[None, :, None]
        + d * np.arange(HALF)[None, None, :]
    ).reshape(-1)
    residues = np.arange(blocks)
    c, s = pair(residues[:, None] * order[None, :], total)
    lanes = np.stack([c, -s], axis=1) * scale
    c, s = pair(residues[:, None] * residues[None, :], blocks)
    folds = np.stack([c, -s], axis=1)[..., None] * np.ones(128)
    lane = np.arange(J)
    slot_of = (lane % HALF) // blocks
    slot = (np.arange(J) // (2 * blocks))[:, None] == slot_of[None, :]
    j = np.arange(HALF)
    b = d * j[None, :] + np.arange(d)[:, None]
    row = np.arange(J)
    lag = (row[None, :, None] - b[:, None, :]) % K
    start = ALT * (j // blocks)
    inside = (row[:, None] - start[None, :]) % K
    late = inside[None] < (b - start[None, :])[:, None, :]
    weight = 0.54 - 0.46 * np.cos(TWO_PI * lag / K)
    weight = np.where(late, -weight, weight)
    chan = np.arange(K)
    c, s = pair(chan[:, None] * row[None, :], K)
    emat = np.stack([np.concatenate([c, s], 1), np.concatenate([-s, c], 1)])
    c, s = pair(chan[:, None] * (d * j)[None, :], K)
    c1, s1 = pair(chan[:, None] * np.ones((1, HALF), np.int64), K)
    phase = np.stack([c, s, c1, s1])
    c, s = pair(row[:, None] * row[None, :], J)
    real, imag = np.concatenate([c, s], 0), np.concatenate([-s, c], 0)
    dft = np.concatenate(
        [part[:, q * HALF : (q + 1) * HALF] for q in range(2) for part in (real, imag)], 1
    )
    twid = np.stack(pair(np.arange(d)[:, None] * row[None, :], block_len))
    f32 = lambda v: np.asarray(v, np.float32)
    b16 = lambda v: np.asarray(np.asarray(v, np.float32), jnp.bfloat16)
    return dict(
        lanes=f32(lanes), folds=f32(folds), slot=b16(slot), weight=b16(weight),
        emat=b16(emat), phase=f32(phase), dft=b16(dft), twid=f32(twid),
    )


def in_hbm(value):
    return pltpu.with_memory_space_constraint(jnp.asarray(value), pltpu.HBM)


def in_vmem(value):
    return pltpu.with_memory_space_constraint(jnp.asarray(value), pltpu.VMEM)


def first_body(names, strips, blocks, wloc, block_len, chan):
    d = block_len // J
    ca = 2 * blocks
    slots = J // ca
    halves = block_len // 2
    pairs = blocks // 2
    lanes_o = J // d
    count = ca * wloc

    def body(
        local_hbm, rows_hbm, lane_hbm, slot_hbm,
        weight_hbm, lanes_hbm, folds_hbm, emat_hbm, phase_hbm, g_ref,
        local_ref, rows_ref, lane_ref, slot_ref,
        every_ref, next_xn_ref, next_zs_ref, xn_ref, zs_ref, lhs_ref,
        signed_ref, weight_ref, taps_ref, lanes_ref, folds_ref, emat_ref, phase_ref, turn_ref, spin_ref,
        load_sem, direct_sem, relay_sem, hand_sem, recv_sem,
    ):
        s = lax.axis_index("strip")
        t = lax.axis_index("tm")
        other = t + 1 - 2 * lax.rem(t, 2)

        def device(strip, tm):
            where = {"strip": strip, "tm": tm}
            return tuple(where[name] for name in names)

        def strip_at(ds):
            return lax.rem(s + strips - ds, strips)

        def mate(dt):
            return lax.rem(t + blocks - 2 * dt, blocks)

        def rival(dt):
            return lax.rem(other + blocks - 2 * dt, blocks)

        across = [device(strip_at(strips - ds), t) for ds in range(1, strips)]
        inside = [device(s, mate(dt)) for dt in range(1, pairs)] + [device(s, other)]
        barrier = pltpu.get_barrier_semaphore()
        for peer in across + inside:
            pl.semaphore_signal(barrier, inc=1, device_id=peer, device_id_type=pl.DeviceIdType.MESH)
        local = pltpu.make_async_copy(local_hbm, local_ref, load_sem.at[8])
        local.start()
        loads = [
            pltpu.make_async_copy(rows_hbm, rows_ref, load_sem.at[5]),
            pltpu.make_async_copy(lane_hbm, lane_ref, load_sem.at[6]),
            pltpu.make_async_copy(slot_hbm, slot_ref, load_sem.at[7]),
            pltpu.make_async_copy(lanes_hbm.at[t], lanes_ref, load_sem.at[0]),
            pltpu.make_async_copy(folds_hbm.at[t], folds_ref, load_sem.at[1]),
            pltpu.make_async_copy(emat_hbm.at[:, pl.ds(s * chan, chan)], emat_ref, load_sem.at[2]),
            pltpu.make_async_copy(phase_hbm.at[:, pl.ds(s * chan, chan)], phase_ref, load_sem.at[3]),
            pltpu.make_async_copy(weight_hbm, signed_ref, load_sem.at[4]),
        ]
        for load in loads:
            load.start()
        local.wait()
        every_ref[s, t] = jnp.concatenate(
            [local_ref[0].astype(jnp.float32), local_ref[1].astype(jnp.float32)], axis=0
        ).astype(jnp.bfloat16)
        pl.semaphore_wait(barrier, len(across) + len(inside))

        def transfer(strip, tm, peer, send_sem):
            return pltpu.make_async_remote_copy(
                src_ref=every_ref.at[strip, tm],
                dst_ref=every_ref.at[strip, tm],
                send_sem=send_sem,
                recv_sem=recv_sem.at[strip, tm],
                device_id=peer,
                device_id_type=pl.DeviceIdType.MESH,
            )

        def arrived(strip, tm):
            transfer(strip, tm, inside[-1], direct_sem.at[0]).wait_recv()

        def direct(i):
            return transfer(s, t, (across + inside)[i], direct_sem.at[i])

        def relay(ds, i):
            return transfer(strip_at(ds), t, inside[i], relay_sem.at[ds, i])

        def hand(ds, dt):
            return transfer(strip_at(ds), mate(dt), inside[-1], hand_sem.at[ds, dt])

        def relay_all(ds):
            arrived(strip_at(ds), t)
            for i in range(len(inside)):
                relay(ds, i).start()

        def hand_over(ds):
            for dt in range(1, pairs):
                arrived(strip_at(ds), mate(dt))
                hand(ds, dt).start()

        def complete(ds):
            for dt in range(pairs):
                arrived(strip_at(ds), rival(dt))

        for i in range(len(inside)):
            direct(len(across) + i).start()
        for i in range(len(across)):
            direct(i).start()

        low = lax.broadcasted_iota(jnp.int32, (ca, HALF), 1) < ALT

        def rows_of(ds):
            flat = every_ref[strip_at(ds)].reshape(count, block_len)
            nat = jnp.dot(rows_ref[0], flat, preferred_element_type=jnp.float32).astype(jnp.bfloat16)
            halo = jnp.dot(rows_ref[1], flat[:, :K], preferred_element_type=jnp.float32).astype(jnp.bfloat16)
            for wl in range(wloc):
                next_xn_ref[wl, :, :block_len] = nat[wl * ca : (wl + 1) * ca]
                next_xn_ref[wl, :, block_len:] = halo[wl * ca : (wl + 1) * ca]
            return jnp.concatenate([nat[:, HALF:], halo[:, :HALF]], axis=1)

        def lanes_of(full):
            moved = jnp.concatenate([full[:, q * J : (q + 1) * J] for q in range(block_len // J)], axis=0)
            moved = jnp.dot(moved, lane_ref[...], preferred_element_type=jnp.float32)
            for h in range(2):
                for o in range(d):
                    lanes = slice(o * lanes_o, (o + 1) * lanes_o)
                    part = jnp.concatenate(
                        [
                            moved[q * count : (q + 1) * count, lanes]
                            for q in range(h * d // 2, (h + 1) * d // 2)
                        ],
                        axis=1,
                    ).astype(jnp.bfloat16)
                    for wl in range(wloc):
                        next_zs_ref[wl, :, (h * d + o) * HALF : (h * d + o + 1) * HALF] = part[
                            wl * ca : (wl + 1) * ca
                        ]

        def build(src_ref, wl, slot):
            def lane_tile(v):
                return src_ref[wl, :, v * 128 : (v + 1) * 128]

            for h in range(2):
                left, right, late = [], [], []
                for part in range(slots):
                    g = (HALF * d * h) // ALT + part
                    picks = [(g + (c - g) % 4) // 2 for c in range(4)]
                    for side, dst in ((0, left), (1, right)):
                        v0, v1 = picks[2 * side], picks[2 * side + 1]
                        x0 = lane_tile(v0)
                        dst.append(x0 if v0 == v1 else jnp.where(low, x0, lane_tile(v1)))
                    n = g + 4
                    tail = lane_tile(n // 2)
                    if n % 2:
                        tail = pltpu.roll(tail.astype(jnp.float32), ALT, 1).astype(jnp.bfloat16)
                    late.append(-tail)
                lhs_ref[slot, h, 0:ALT] = jnp.concatenate(late, axis=0).T[:ALT]
                lhs_ref[slot, h, ALT : ALT + HALF] = jnp.concatenate(left, axis=0).T
                lhs_ref[slot, h, ALT + HALF :] = jnp.concatenate(right, axis=0).T

        def lag_products(wl, h, o):
            at = slice(h * halves + o * HALF, h * halves + (o + 2) * HALF)
            xs = zs_ref[wl, :, at].astype(jnp.float32)
            xr, xi = xs[:blocks], xs[blocks:]
            er, ei = turn_ref[0, :, at], turn_ref[1, :, at]
            zr = xr * er + xi * ei
            zi = xr * ei - xi * er
            mask = slot_ref[...]
            zre = jnp.concatenate([zr, -zi], axis=0).astype(jnp.bfloat16)
            zim = jnp.concatenate([zi, zr], axis=0).astype(jnp.bfloat16)
            rhs = jnp.concatenate(
                [
                    jnp.concatenate([zre] * slots, axis=0) * mask,
                    jnp.concatenate([zim] * slots, axis=0) * mask,
                ],
                axis=1,
            )
            return jnp.dot(lhs_ref[wl % 2, h], rhs, preferred_element_type=jnp.float32)

        def weigh(o, lags):
            cols = []
            for c in range(2):
                for oo in range(2):
                    lanes = slice(c * J + oo * HALF, c * J + (oo + 1) * HALF)
                    late = lags[:ALT, lanes].astype(jnp.bfloat16)
                    parts = []
                    for q in range(4):
                        at = slice(q * ALT, (q + 1) * ALT)
                        early = lags[(q + 1) * ALT : (q + 2) * ALT, lanes].astype(jnp.bfloat16)
                        parts.append(early * weight_ref[o + oo, 0, at] + late * weight_ref[o + oo, 1, at])
                    cols.append(jnp.concatenate(parts, axis=0))
            return jnp.concatenate(
                [jnp.concatenate(cols[:2], axis=1), jnp.concatenate(cols[2:], axis=1)], axis=0
            )

        def channels(ds, wl, h, o, taps):
            w = strip_at(ds) * wloc + wl
            emat = emat_ref[...].reshape(2 * chan, 2 * J)
            y = jnp.dot(emat, taps, preferred_element_type=jnp.float32)
            for oo in range(2):
                lanes = slice(oo * HALF, (oo + 1) * HALF)
                yr, yi = y[:chan, lanes], y[chan:, lanes]
                c, sn = spin_ref[o + oo, 0], spin_ref[o + oo, 1]
                gr = (yr * c - yi * sn).astype(jnp.bfloat16).reshape(chan // GROUP, GROUP, HALF)
                gi = (yr * sn + yi * c).astype(jnp.bfloat16).reshape(chan // GROUP, GROUP, HALF)
                g_ref[:, w, o + oo, :, h * HALF : (h + 1) * HALF] = gr
                g_ref[:, w, o + oo, :, J + h * HALF : J + (h + 1) * HALF] = gi

        for load in loads:
            load.wait()
        for o in range(d):
            signed = signed_ref[o].astype(jnp.float32)
            weight_ref[o, 0] = jnp.maximum(signed, 0.0).astype(jnp.bfloat16)
            weight_ref[o, 1] = jnp.minimum(signed, 0.0).astype(jnp.bfloat16)
        br, bi = lanes_ref[0:1], lanes_ref[1:2]
        for q in range(block_len // 128):
            at = slice(q * 128, (q + 1) * 128)
            fr, fi = folds_ref[0], folds_ref[1]
            turn_ref[0, :, at] = fr * br[:, at] - fi * bi[:, at]
            turn_ref[1, :, at] = fr * bi[:, at] + fi * br[:, at]
        gr, gi = phase_ref[0], phase_ref[1]
        for o in range(d):
            if o > 0:
                gr, gi = gr * phase_ref[2] - gi * phase_ref[3], gr * phase_ref[3] + gi * phase_ref[2]
            spin_ref[o, 0] = gr
            spin_ref[o, 1] = gi

        near = [1, strips - 1] if strips > 2 else [1]
        far = [ds for ds in range(1, strips) if ds not in near]
        hand_over(0)
        for ds in near + far:
            relay_all(ds)
        taps_ref[...] = jnp.zeros((2 * J, J), jnp.bfloat16)
        complete(0)
        lanes_of(rows_of(0))
        build(next_xn_ref, 0, 0)

        @pl.loop(0, strips)
        def _(ds):
            xn_ref[...] = next_xn_ref[...]
            zs_ref[...] = next_zs_ref[...]
            after = jnp.minimum(ds + 1, strips - 1)

            @pl.when(ds + 1 < strips)
            def _():
                hand_over(ds + 1)

            for first in range(0, wloc, UNROLL):
                last = first + UNROLL >= wloc
                mine = range(first, min(first + UNROLL, wloc))

                if last:

                    @pl.when(ds + 1 < strips)
                    def _():
                        complete(ds + 1)

                    full = rows_of(after)
                pending = None
                for wl in mine:
                    if wl + 1 < wloc:
                        build(xn_ref, wl + 1, (wl + 1) % 2)
                    else:
                        build(next_xn_ref, 0, 0)
                    for h in range(2):
                        for o in range(0, d, 2):
                            lags = lag_products(wl, h, o)
                            if pending is not None:
                                channels(ds, *pending[:3], weigh(*pending[2:]))
                            elif first > 0:
                                channels(ds, first - 1, 1, d - 2, taps_ref[...])
                            else:
                                channels(ds - 1, wloc - 1, 1, d - 2, taps_ref[...])
                            pending = (wl, h, o, lags)
                        if last and wl == first and h == 0:
                            lanes_of(full)
                taps_ref[...] = weigh(*pending[2:])

        channels(strips - 1, wloc - 1, 1, d - 2, taps_ref[...])
        for i in range(len(across) + len(inside)):
            direct(i).wait_send()
        for ds in range(strips):
            if ds > 0:
                for i in range(len(inside)):
                    relay(ds, i).wait_send()
            for dt in range(1, pairs):
                hand(ds, dt).wait_send()

    return body


def arrangements(blocks, wloc, d):
    count = 2 * blocks * wloc
    w, c, a = np.meshgrid(np.arange(wloc), np.arange(2), np.arange(blocks), indexing="ij")
    target = ((w * 2 + c) * blocks + a).reshape(-1)
    source = ((a * 2 + c) * wloc + w).reshape(-1)
    rows = np.zeros((2, count, count))
    rows[0, target, source] = 1.0
    inner = a.reshape(-1) + 1 < blocks
    rows[1, target[inner], source[inner] + 2 * wloc] = 1.0
    lane = np.zeros((J, J))
    n = np.arange(J)
    lane[n, (n % d) * (J // d) + n // d] = 1.0
    return np.asarray(rows, jnp.bfloat16), np.asarray(lane, jnp.bfloat16)


def first_phase(signal, tab, names, strips, blocks):
    wloc, block_len = signal.shape[1], signal.shape[2]
    d = block_len // J
    chan = K // strips
    windows = wloc * strips
    ca = 2 * blocks
    rows, lane = arrangements(blocks, wloc, d)
    hbm = pl.BlockSpec(memory_space=pltpu.HBM)
    b16, f32 = jnp.bfloat16, jnp.float32
    peers = strips - 1 + blocks // 2
    return pl.pallas_call(
        first_body(names, strips, blocks, wloc, block_len, chan),
        out_shape=pltpu.VMEM((chan // GROUP, windows, d, GROUP, 2 * J), b16),
        in_specs=[hbm] * 9,
        out_specs=pl.BlockSpec(memory_space=pltpu.VMEM),
        scratch_shapes=[
            pltpu.VMEM((2, wloc, block_len), b16),
            pltpu.VMEM((2, ca * wloc, ca * wloc), b16),
            pltpu.VMEM((J, J), b16),
            pltpu.VMEM((J, J), b16),
            pltpu.VMEM((strips, blocks, 2 * wloc, block_len), b16),
            pltpu.VMEM((wloc, ca, block_len + K), b16),
            pltpu.VMEM((wloc, ca, block_len), b16),
            pltpu.VMEM((wloc, ca, block_len + K), b16),
            pltpu.VMEM((wloc, ca, block_len), b16),
            pltpu.VMEM((2, 2, ALT + J, J), b16),
            pltpu.VMEM((d, J, HALF), b16),
            pltpu.VMEM((d, 2, J, HALF), b16),
            pltpu.VMEM((2 * J, J), b16),
            pltpu.VMEM((2, block_len), f32),
            pltpu.VMEM((2, blocks, 128), f32),
            pltpu.VMEM((2, chan, 2 * J), b16),
            pltpu.VMEM((4, chan, HALF), f32),
            pltpu.VMEM((2, blocks, block_len), f32),
            pltpu.VMEM((d, 2, chan, HALF), f32),
            pltpu.SemaphoreType.DMA((9,)),
            pltpu.SemaphoreType.DMA((peers,)),
            pltpu.SemaphoreType.DMA((strips, blocks // 2)),
            pltpu.SemaphoreType.DMA((strips, blocks // 2)),
            pltpu.SemaphoreType.DMA((strips, blocks)),
        ],
        compiler_params=pltpu.CompilerParams(
            collective_id=0, has_side_effects=True, vmem_limit_bytes=24 * 1024 * 1024
        ),
        name="lag_channels",
    )(*map(in_hbm, (signal, rows, lane, tab["slot"], tab["weight"], tab["lanes"], tab["folds"], tab["emat"], tab["phase"])))


def final_body(chunks, windows, block_len):
    d = block_len // J
    pitch = GROUP + 1
    step = 4
    span = 8
    unroll = 4 if chunks % 4 == 0 else 1

    def body(g_ref, dft_ref, twid_ref, out_hbm, out_ref, y_ref, out_sem):
        def write(i):
            at = pl.ds(i * GROUP, GROUP)
            return pltpu.make_async_copy(out_ref.at[:, at], out_hbm.at[:, at], out_sem.at[i])

        def windows_of(i, u, w0):
            count = step * GROUP
            lhs = jnp.concatenate(
                [g_ref[i, w0 : w0 + step, o].reshape(count, 2 * J) for o in range(d)], axis=0
            )
            for q in range(2):
                inner = jnp.dot(
                    lhs, dft_ref[:, q * J : (q + 1) * J], preferred_element_type=jnp.float32
                )
                turned = []
                for o in range(d):
                    vr = inner[o * count : (o + 1) * count, :HALF]
                    vi = inner[o * count : (o + 1) * count, HALF:]
                    if o > 0:
                        at = slice(q * HALF, (q + 1) * HALF)
                        tc, ts = twid_ref[0, o : o + 1, at], twid_ref[1, o : o + 1, at]
                        vr, vi = vr * tc + vi * ts, vi * tc - vr * ts
                    turned.append((vr, vi))
                for m, both in enumerate(small_dft(turned)):
                    for c in range(2):
                        for wi in range(step):
                            y_ref[u, c, m * 2 + q, pl.ds((w0 + wi) * pitch, GROUP), :] = both[c][
                                wi * GROUP : (wi + 1) * GROUP
                            ]
            if (w0 + step) % span == 0:
                w1 = w0 + step - span
                for k in range(GROUP):
                    for c in range(2):
                        for q in range(block_len // 128):
                            out_ref[c, i * GROUP + k, w1 : w1 + span, q * 128 : (q + 1) * 128] = y_ref[
                                u, c, q, pl.ds(w1 * pitch + k, span, stride=pitch), :
                            ].astype(jnp.bfloat16)

        @pl.loop(0, chunks // unroll)
        def _(n):
            for u in range(unroll):
                for w0 in range(0, windows, step):
                    windows_of(n * unroll + u, u % 2, w0)
                write(n * unroll + u).start()

        @pl.loop(0, chunks)
        def _(i):
            write(i).wait()

    return body


def final_phase(g, tab):
    chunks, windows, d, _, wide = g.shape
    block_len = d * J
    chan = chunks * GROUP
    hbm = pl.BlockSpec(memory_space=pltpu.HBM)
    b16, f32 = jnp.bfloat16, jnp.float32
    return pl.pallas_call(
        final_body(chunks, windows, block_len),
        in_specs=[pl.BlockSpec(memory_space=pltpu.VMEM)] * 3,
        out_specs=hbm,
        out_shape=jax.ShapeDtypeStruct((2, chan, windows, block_len), b16),
        scratch_shapes=[
            pltpu.VMEM((2, chan, windows, block_len), b16),
            pltpu.VMEM((2, 2, block_len // 128, windows * (GROUP + 1), 128), f32),
            pltpu.SemaphoreType.DMA((chunks,)),
        ],
        compiler_params=pltpu.CompilerParams(vmem_limit_bytes=28 * 1024 * 1024),
        name="frequencies",
    )(*map(in_vmem, (g, tab["dft"], tab["twid"])))


def per_device(names, signal):
    blocks = lax.axis_size("tm")
    strips = lax.axis_size("strip")
    wloc, block_len = signal.shape[1], signal.shape[2]
    tab = tables(blocks, block_len)
    g = first_phase(signal, tab, names, strips, blocks)
    out = final_phase(g, tab)
    return out.reshape(2, K // strips, wloc * strips, 1, block_len)


def solution(mesh):
    return jax.shard_map(
        functools.partial(per_device, tuple(mesh.axis_names)),
        mesh=mesh,
        in_specs=(P(None, "strip", "tm"),),
        out_specs=P(None, "strip", None, "tm", None),
        check_vma=False,
    )
```

```python
import functools
import math

import jax
import jax.numpy as jnp
import numpy as np
from jax import lax
from jax.experimental import pallas as pl
from jax.experimental.pallas import tpu as pltpu
from jax.sharding import PartitionSpec as P

K = 256
J = 256
HALF = 128
ALT = 64
UNROLL = 2
GROUP = 8
TWO_PI = 2.0 * math.pi


def pair(phases, modulus):
    angles = TWO_PI * (phases % modulus) / modulus
    return np.cos(angles), np.sin(angles)


def small_dft(values):
    count = len(values)
    if count == 1:
        return values
    even = small_dft(values[0::2])
    odd = small_dft(values[1::2])
    low, high = [], []
    for i in range(count // 2):
        er, ei = even[i]
        orr, oi = odd[i]
        if i == 0:
            tr, ti = orr, oi
        elif 4 * i == count:
            tr, ti = oi, -orr
        else:
            c = math.cos(TWO_PI * i / count)
            s = math.sin(TWO_PI * i / count)
            if abs(c - s) < 1e-6:
                tr, ti = (orr + oi) * c, (oi - orr) * c
            elif abs(c + s) < 1e-6:
                tr, ti = (oi - orr) * s, (orr + oi) * (-s)
            else:
                tr, ti = orr * c + oi * s, oi * c - orr * s
        low.append((er + tr, ei + ti))
        high.append((er - tr, ei - ti))
    return low + high


def tables(blocks, block_len):
    d = block_len // J
    slots = J // (2 * blocks)
    total = blocks * block_len
    scale = 1.0 / math.sqrt(total * K)
    order = (
        HALF * d * np.arange(2)[:, None, None]
        + np.arange(d)[None, :, None]
        + d * np.arange(HALF)[None, None, :]
    ).reshape(-1)
    residues = np.arange(blocks)
    c, s = pair(residues[:, None] * order[None, :], total)
    lanes = np.stack([c, -s], axis=1) * scale
    c, s = pair(residues[:, None] * residues[None, :], blocks)
    folds = np.stack([c, -s], axis=1)[..., None] * np.ones(128)
    lane = np.arange(J)
    slot_of = (lane % HALF) // blocks
    slot = (np.arange(J) // (2 * blocks))[:, None] == slot_of[None, :]
    j = np.arange(HALF)
    b = d * j[None, :] + np.arange(d)[:, None]
    row = np.arange(J)
    lag = (row[None, :, None] - b[:, None, :]) % K
    start = ALT * (j // blocks)
    inside = (row[:, None] - start[None, :]) % K
    late = inside[None] < (b - start[None, :])[:, None, :]
    weight = 0.54 - 0.46 * np.cos(TWO_PI * lag / K)
    weight = np.where(late, -weight, weight)
    chan = np.arange(K)
    c, s = pair(chan[:, None] * row[None, :], K)
    emat = np.stack([np.concatenate([c, s], 1), np.concatenate([-s, c], 1)])
    c, s = pair(chan[:, None] * (d * j)[None, :], K)
    c1, s1 = pair(chan[:, None] * np.ones((1, HALF), np.int64), K)
    phase = np.stack([c, s, c1, s1])
    c, s = pair(row[:, None] * row[None, :], J)
    real, imag = np.concatenate([c, s], 0), np.concatenate([-s, c], 0)
    dft = np.concatenate(
        [part[:, q * HALF : (q + 1) * HALF] for q in range(2) for part in (real, imag)], 1
    )
    twid = np.stack(pair(np.arange(d)[:, None] * row[None, :], block_len))
    f32 = lambda v: np.asarray(v, np.float32)
    b16 = lambda v: np.asarray(np.asarray(v, np.float32), jnp.bfloat16)
    return dict(
        lanes=f32(lanes), folds=f32(folds), slot=b16(slot), weight=b16(weight),
        emat=b16(emat), phase=f32(phase), dft=b16(dft), twid=f32(twid),
    )


def in_hbm(value):
    return pltpu.with_memory_space_constraint(jnp.asarray(value), pltpu.HBM)


def in_vmem(value):
    return pltpu.with_memory_space_constraint(jnp.asarray(value), pltpu.VMEM)


def first_body(names, strips, blocks, wloc, block_len, chan):
    d = block_len // J
    ca = 2 * blocks
    slots = J // ca
    halves = block_len // 2
    pairs = blocks // 2
    lanes_o = J // d
    count = ca * wloc

    def body(
        local_hbm, rows_hbm, lane_hbm, slot_hbm,
        weight_hbm, lanes_hbm, folds_hbm, emat_hbm, phase_hbm, g_ref,
        local_ref, rows_ref, lane_ref, slot_ref,
        every_ref, next_xn_ref, next_zs_ref, xn_ref, zs_ref, lhs_ref,
        signed_ref, weight_ref, taps_ref, lanes_ref, folds_ref, emat_ref, phase_ref, turn_ref, spin_ref,
        load_sem, direct_sem, relay_sem, hand_sem, recv_sem,
    ):
        s = lax.axis_index("strip")
        t = lax.axis_index("tm")
        other = t + 1 - 2 * lax.rem(t, 2)

        def device(strip, tm):
            where = {"strip": strip, "tm": tm}
            return tuple(where[name] for name in names)

        def strip_at(ds):
            return lax.rem(s + strips - ds, strips)

        def mate(dt):
            return lax.rem(t + blocks - 2 * dt, blocks)

        def rival(dt):
            return lax.rem(other + blocks - 2 * dt, blocks)

        across = [device(strip_at(strips - ds), t) for ds in range(1, strips)]
        inside = [device(s, mate(dt)) for dt in range(1, pairs)] + [device(s, other)]
        barrier = pltpu.get_barrier_semaphore()
        for peer in across + inside:
            pl.semaphore_signal(barrier, inc=1, device_id=peer, device_id_type=pl.DeviceIdType.MESH)
        local = pltpu.make_async_copy(local_hbm, local_ref, load_sem.at[8])
        local.start()
        loads = [
            pltpu.make_async_copy(rows_hbm, rows_ref, load_sem.at[5]),
            pltpu.make_async_copy(lane_hbm, lane_ref, load_sem.at[6]),
            pltpu.make_async_copy(slot_hbm, slot_ref, load_sem.at[7]),
            pltpu.make_async_copy(lanes_hbm.at[t], lanes_ref, load_sem.at[0]),
            pltpu.make_async_copy(folds_hbm.at[t], folds_ref, load_sem.at[1]),
            pltpu.make_async_copy(emat_hbm.at[:, pl.ds(s * chan, chan)], emat_ref, load_sem.at[2]),
            pltpu.make_async_copy(phase_hbm.at[:, pl.ds(s * chan, chan)], phase_ref, load_sem.at[3]),
            pltpu.make_async_copy(weight_hbm, signed_ref, load_sem.at[4]),
        ]
        for load in loads:
            load.start()
        local.wait()
        every_ref[s, t] = jnp.concatenate(
            [local_ref[0].astype(jnp.float32), local_ref[1].astype(jnp.float32)], axis=0
        ).astype(jnp.bfloat16)
        pl.semaphore_wait(barrier, len(across) + len(inside))

        def transfer(strip, tm, peer, send_sem):
            return pltpu.make_async_remote_copy(
                src_ref=every_ref.at[strip, tm],
                dst_ref=every_ref.at[strip, tm],
                send_sem=send_sem,
                recv_sem=recv_sem.at[strip, tm],
                device_id=peer,
                device_id_type=pl.DeviceIdType.MESH,
            )

        def arrived(strip, tm):
            transfer(strip, tm, inside[-1], direct_sem.at[0]).wait_recv()

        def direct(i):
            return transfer(s, t, (across + inside)[i], direct_sem.at[i])

        def relay(ds, i):
            return transfer(strip_at(ds), t, inside[i], relay_sem.at[ds, i])

        def hand(ds, dt):
            return transfer(strip_at(ds), mate(dt), inside[-1], hand_sem.at[ds, dt])

        def relay_all(ds):
            arrived(strip_at(ds), t)
            for i in range(len(inside)):
                relay(ds, i).start()

        def hand_over(ds):
            for dt in range(1, pairs):
                arrived(strip_at(ds), mate(dt))
                hand(ds, dt).start()

        def complete(ds):
            for dt in range(pairs):
                arrived(strip_at(ds), rival(dt))

        for i in range(len(inside)):
            direct(len(across) + i).start()
        for i in range(len(across)):
            direct(i).start()

        low = lax.broadcasted_iota(jnp.int32, (ca, HALF), 1) < ALT

        def rows_of(ds):
            flat = every_ref[strip_at(ds)].reshape(count, block_len)
            nat = jnp.dot(rows_ref[0], flat, preferred_element_type=jnp.float32).astype(jnp.bfloat16)
            halo = jnp.dot(rows_ref[1], flat[:, :K], preferred_element_type=jnp.float32).astype(jnp.bfloat16)
            for wl in range(wloc):
                next_xn_ref[wl, :, :block_len] = nat[wl * ca : (wl + 1) * ca]
                next_xn_ref[wl, :, block_len:] = halo[wl * ca : (wl + 1) * ca]
            return jnp.concatenate([nat[:, HALF:], halo[:, :HALF]], axis=1)

        def lanes_of(full):
            moved = jnp.concatenate([full[:, q * J : (q + 1) * J] for q in range(block_len // J)], axis=0)
            moved = jnp.dot(moved, lane_ref[...], preferred_element_type=jnp.float32)
            for h in range(2):
                for o in range(d):
                    lanes = slice(o * lanes_o, (o + 1) * lanes_o)
                    part = jnp.concatenate(
                        [
                            moved[q * count : (q + 1) * count, lanes]
                            for q in range(h * d // 2, (h + 1) * d // 2)
                        ],
                        axis=1,
                    ).astype(jnp.bfloat16)
                    for wl in range(wloc):
                        next_zs_ref[wl, :, (h * d + o) * HALF : (h * d + o + 1) * HALF] = part[
                            wl * ca : (wl + 1) * ca
                        ]

        def build(src_ref, wl, slot):
            def lane_tile(v):
                return src_ref[wl, :, v * 128 : (v + 1) * 128]

            for h in range(2):
                left, right, late = [], [], []
                for part in range(slots):
                    g = (HALF * d * h) // ALT + part
                    picks = [(g + (c - g) % 4) // 2 for c in range(4)]
                    for side, dst in ((0, left), (1, right)):
                        v0, v1 = picks[2 * side], picks[2 * side + 1]
                        x0 = lane_tile(v0)
                        dst.append(x0 if v0 == v1 else jnp.where(low, x0, lane_tile(v1)))
                    n = g + 4
                    tail = lane_tile(n // 2)
                    if n % 2:
                        tail = pltpu.roll(tail.astype(jnp.float32), ALT, 1).astype(jnp.bfloat16)
                    late.append(-tail)
                lhs_ref[slot, h, 0:ALT] = jnp.concatenate(late, axis=0).T[:ALT]
                lhs_ref[slot, h, ALT : ALT + HALF] = jnp.concatenate(left, axis=0).T
                lhs_ref[slot, h, ALT + HALF :] = jnp.concatenate(right, axis=0).T

        def lag_products(wl, h, o):
            at = slice(h * halves + o * HALF, h * halves + (o + 2) * HALF)
            xs = zs_ref[wl, :, at].astype(jnp.float32)
            xr, xi = xs[:blocks], xs[blocks:]
            er, ei = turn_ref[0, :, at], turn_ref[1, :, at]
            zr = xr * er + xi * ei
            zi = xr * ei - xi * er
            mask = slot_ref[...]
            zre = jnp.concatenate([zr, -zi], axis=0).astype(jnp.bfloat16)
            zim = jnp.concatenate([zi, zr], axis=0).astype(jnp.bfloat16)
            rhs = jnp.concatenate(
                [
                    jnp.concatenate([zre] * slots, axis=0) * mask,
                    jnp.concatenate([zim] * slots, axis=0) * mask,
                ],
                axis=1,
            )
            return jnp.dot(lhs_ref[wl % 2, h], rhs, preferred_element_type=jnp.float32)

        def weigh(o, lags):
            cols = []
            for c in range(2):
                for oo in range(2):
                    lanes = slice(c * J + oo * HALF, c * J + (oo + 1) * HALF)
                    late = lags[:ALT, lanes].astype(jnp.bfloat16)
                    parts = []
                    for q in range(4):
                        at = slice(q * ALT, (q + 1) * ALT)
                        early = lags[(q + 1) * ALT : (q + 2) * ALT, lanes].astype(jnp.bfloat16)
                        parts.append(early * weight_ref[o + oo, 0, at] + late * weight_ref[o + oo, 1, at])
                    cols.append(jnp.concatenate(parts, axis=0))
            return jnp.concatenate(
                [jnp.concatenate(cols[:2], axis=1), jnp.concatenate(cols[2:], axis=1)], axis=0
            )

        def channels(ds, wl, h, o, taps):
            w = strip_at(ds) * wloc + wl
            emat = emat_ref[...].reshape(2 * chan, 2 * J)
            y = jnp.dot(emat, taps, preferred_element_type=jnp.float32)
            for oo in range(2):
                lanes = slice(oo * HALF, (oo + 1) * HALF)
                yr, yi = y[:chan, lanes], y[chan:, lanes]
                c, sn = spin_ref[o + oo, 0], spin_ref[o + oo, 1]
                gr = (yr * c - yi * sn).astype(jnp.bfloat16).reshape(chan // GROUP, GROUP, HALF)
                gi = (yr * sn + yi * c).astype(jnp.bfloat16).reshape(chan // GROUP, GROUP, HALF)
                g_ref[:, w, o + oo, :, h * HALF : (h + 1) * HALF] = gr
                g_ref[:, w, o + oo, :, J + h * HALF : J + (h + 1) * HALF] = gi

        for load in loads:
            load.wait()
        for o in range(d):
            signed = signed_ref[o].astype(jnp.float32)
            weight_ref[o, 0] = jnp.maximum(signed, 0.0).astype(jnp.bfloat16)
            weight_ref[o, 1] = jnp.minimum(signed, 0.0).astype(jnp.bfloat16)
        br, bi = lanes_ref[0:1], lanes_ref[1:2]
        for q in range(block_len // 128):
            at = slice(q * 128, (q + 1) * 128)
            fr, fi = folds_ref[0], folds_ref[1]
            turn_ref[0, :, at] = fr * br[:, at] - fi * bi[:, at]
            turn_ref[1, :, at] = fr * bi[:, at] + fi * br[:, at]
        gr, gi = phase_ref[0], phase_ref[1]
        for o in range(d):
            if o > 0:
                gr, gi = gr * phase_ref[2] - gi * phase_ref[3], gr * phase_ref[3] + gi * phase_ref[2]
            spin_ref[o, 0] = gr
            spin_ref[o, 1] = gi

        near = [1, strips - 1] if strips > 2 else [1]
        far = [ds for ds in range(1, strips) if ds not in near]
        hand_over(0)
        for ds in near + far:
            relay_all(ds)
        taps_ref[...] = jnp.zeros((2 * J, J), jnp.bfloat16)
        complete(0)
        lanes_of(rows_of(0))
        build(next_xn_ref, 0, 0)

        @pl.loop(0, strips)
        def _(ds):
            xn_ref[...] = next_xn_ref[...]
            zs_ref[...] = next_zs_ref[...]
            after = jnp.minimum(ds + 1, strips - 1)

            @pl.when(ds + 1 < strips)
            def _():
                hand_over(ds + 1)

            for first in range(0, wloc, UNROLL):
                last = first + UNROLL >= wloc
                mine = range(first, min(first + UNROLL, wloc))

                if last:

                    @pl.when(ds + 1 < strips)
                    def _():
                        complete(ds + 1)

                    full = rows_of(after)
                pending = None
                for wl in mine:
                    if wl + 1 < wloc:
                        build(xn_ref, wl + 1, (wl + 1) % 2)
                    else:
                        build(next_xn_ref, 0, 0)
                    for h in range(2):
                        for o in range(0, d, 2):
                            lags = lag_products(wl, h, o)
                            if pending is not None:
                                channels(ds, *pending[:3], weigh(*pending[2:]))
                            elif first > 0:
                                channels(ds, first - 1, 1, d - 2, taps_ref[...])
                            else:
                                channels(ds - 1, wloc - 1, 1, d - 2, taps_ref[...])
                            pending = (wl, h, o, lags)
                        if last and wl == first and h == 0:
                            lanes_of(full)
                taps_ref[...] = weigh(*pending[2:])

        channels(strips - 1, wloc - 1, 1, d - 2, taps_ref[...])
        for i in range(len(across) + len(inside)):
            direct(i).wait_send()
        for ds in range(strips):
            if ds > 0:
                for i in range(len(inside)):
                    relay(ds, i).wait_send()
            for dt in range(1, pairs):
                hand(ds, dt).wait_send()

    return body


def arrangements(blocks, wloc, d):
    count = 2 * blocks * wloc
    w, c, a = np.meshgrid(np.arange(wloc), np.arange(2), np.arange(blocks), indexing="ij")
    target = ((w * 2 + c) * blocks + a).reshape(-1)
    source = ((a * 2 + c) * wloc + w).reshape(-1)
    rows = np.zeros((2, count, count))
    rows[0, target, source] = 1.0
    inner = a.reshape(-1) + 1 < blocks
    rows[1, target[inner], source[inner] + 2 * wloc] = 1.0
    lane = np.zeros((J, J))
    n = np.arange(J)
    lane[n, (n % d) * (J // d) + n // d] = 1.0
    return np.asarray(rows, jnp.bfloat16), np.asarray(lane, jnp.bfloat16)


def first_phase(signal, tab, names, strips, blocks):
    wloc, block_len = signal.shape[1], signal.shape[2]
    d = block_len // J
    chan = K // strips
    windows = wloc * strips
    ca = 2 * blocks
    rows, lane = arrangements(blocks, wloc, d)
    hbm = pl.BlockSpec(memory_space=pltpu.HBM)
    b16, f32 = jnp.bfloat16, jnp.float32
    peers = strips - 1 + blocks // 2
    return pl.pallas_call(
        first_body(names, strips, blocks, wloc, block_len, chan),
        out_shape=pltpu.VMEM((chan // GROUP, windows, d, GROUP, 2 * J), b16),
        in_specs=[hbm] * 9,
        out_specs=pl.BlockSpec(memory_space=pltpu.VMEM),
        scratch_shapes=[
            pltpu.VMEM((2, wloc, block_len), b16),
            pltpu.VMEM((2, ca * wloc, ca * wloc), b16),
            pltpu.VMEM((J, J), b16),
            pltpu.VMEM((J, J), b16),
            pltpu.VMEM((strips, blocks, 2 * wloc, block_len), b16),
            pltpu.VMEM((wloc, ca, block_len + K), b16),
            pltpu.VMEM((wloc, ca, block_len), b16),
            pltpu.VMEM((wloc, ca, block_len + K), b16),
            pltpu.VMEM((wloc, ca, block_len), b16),
            pltpu.VMEM((2, 2, ALT + J, J), b16),
            pltpu.VMEM((d, J, HALF), b16),
            pltpu.VMEM((d, 2, J, HALF), b16),
            pltpu.VMEM((2 * J, J), b16),
            pltpu.VMEM((2, block_len), f32),
            pltpu.VMEM((2, blocks, 128), f32),
            pltpu.VMEM((2, chan, 2 * J), b16),
            pltpu.VMEM((4, chan, HALF), f32),
            pltpu.VMEM((2, blocks, block_len), f32),
            pltpu.VMEM((d, 2, chan, HALF), f32),
            pltpu.SemaphoreType.DMA((9,)),
            pltpu.SemaphoreType.DMA((peers,)),
            pltpu.SemaphoreType.DMA((strips, blocks // 2)),
            pltpu.SemaphoreType.DMA((strips, blocks // 2)),
            pltpu.SemaphoreType.DMA((strips, blocks)),
        ],
        compiler_params=pltpu.CompilerParams(
            collective_id=0, has_side_effects=True, vmem_limit_bytes=24 * 1024 * 1024
        ),
        name="lag_channels",
    )(*map(in_hbm, (signal, rows, lane, tab["slot"], tab["weight"], tab["lanes"], tab["folds"], tab["emat"], tab["phase"])))


def final_body(chunks, windows, block_len):
    d = block_len // J
    pitch = GROUP + 1
    step = 8
    span = 8
    unroll = 4 if chunks % 4 == 0 else 1

    def body(g_ref, dft_ref, twid_ref, out_hbm, out_ref, y_ref, out_sem):
        def write(i):
            at = pl.ds(i * GROUP, GROUP)
            return pltpu.make_async_copy(out_ref.at[:, at], out_hbm.at[:, at], out_sem.at[i])

        def windows_of(i, u, w0):
            count = step * GROUP
            lhs = jnp.concatenate(
                [g_ref[i, w0 : w0 + step, o].reshape(count, 2 * J) for o in range(d)], axis=0
            )
            for q in range(2):
                inner = jnp.dot(
                    lhs, dft_ref[:, q * J : (q + 1) * J], preferred_element_type=jnp.float32
                )
                turned = []
                for o in range(d):
                    vr = inner[o * count : (o + 1) * count, :HALF]
                    vi = inner[o * count : (o + 1) * count, HALF:]
                    if o > 0:
                        at = slice(q * HALF, (q + 1) * HALF)
                        tc, ts = twid_ref[0, o : o + 1, at], twid_ref[1, o : o + 1, at]
                        vr, vi = vr * tc + vi * ts, vi * tc - vr * ts
                    turned.append((vr, vi))
                for m, both in enumerate(small_dft(turned)):
                    for c in range(2):
                        for wi in range(step):
                            y_ref[u, c, m * 2 + q, pl.ds((w0 + wi) * pitch, GROUP), :] = both[c][
                                wi * GROUP : (wi + 1) * GROUP
                            ]
            if (w0 + step) % span == 0:
                w1 = w0 + step - span
                for k in range(GROUP):
                    for c in range(2):
                        for q in range(block_len // 128):
                            out_ref[c, i * GROUP + k, w1 : w1 + span, q * 128 : (q + 1) * 128] = y_ref[
                                u, c, q, pl.ds(w1 * pitch + k, span, stride=pitch), :
                            ].astype(jnp.bfloat16)

        @pl.loop(0, chunks // unroll)
        def _(n):
            for u in range(unroll):
                for w0 in range(0, windows, step):
                    windows_of(n * unroll + u, u % 2, w0)
                write(n * unroll + u).start()

        @pl.loop(0, chunks)
        def _(i):
            write(i).wait()

    return body


def final_phase(g, tab):
    chunks, windows, d, _, wide = g.shape
    block_len = d * J
    chan = chunks * GROUP
    hbm = pl.BlockSpec(memory_space=pltpu.HBM)
    b16, f32 = jnp.bfloat16, jnp.float32
    return pl.pallas_call(
        final_body(chunks, windows, block_len),
        in_specs=[pl.BlockSpec(memory_space=pltpu.VMEM)] * 3,
        out_specs=hbm,
        out_shape=jax.ShapeDtypeStruct((2, chan, windows, block_len), b16),
        scratch_shapes=[
            pltpu.VMEM((2, chan, windows, block_len), b16),
            pltpu.VMEM((2, 2, block_len // 128, windows * (GROUP + 1), 128), f32),
            pltpu.SemaphoreType.DMA((chunks,)),
        ],
        compiler_params=pltpu.CompilerParams(vmem_limit_bytes=28 * 1024 * 1024),
        name="frequencies",
    )(*map(in_vmem, (g, tab["dft"], tab["twid"])))


def per_device(names, signal):
    blocks = lax.axis_size("tm")
    strips = lax.axis_size("strip")
    wloc, block_len = signal.shape[1], signal.shape[2]
    tab = tables(blocks, block_len)
    g = first_phase(signal, tab, names, strips, blocks)
    out = final_phase(g, tab)
    return out.reshape(2, K // strips, wloc * strips, 1, block_len)


def solution(mesh):
    return jax.shard_map(
        functools.partial(per_device, tuple(mesh.axis_names)),
        mesh=mesh,
        in_specs=(P(None, "strip", "tm"),),
        out_specs=P(None, "strip", None, "tm", None),
        check_vma=False,
    )
```
